128 devices in a mesh: rep: 2 (over core), dp: 64 (over x, y, z).
Axes of the slice: x: 4, y: 4, z: 4, core: 2. Of those that a mesh axis runs over, the one named last changes fastest.
Arguments:
- x: bfloat16 [128, 2048, 896], P(('rep', 'dp')), parts along dimension 0
- dy: bfloat16 [128, 2048, 896], P(('rep', 'dp')), parts along dimension 0
- w_gate: bfloat16 [2, 896, 2560], P(None, 'dp')
- w_up: bfloat16 [2, 896, 2560], P(None, 'dp')
- w_down: bfloat16 [2, 2560, 896], P(None, 'dp')
Outputs:
- output 1: bfloat16 [128, 2048, 896], P(('rep', 'dp')), parts along dimension 0
- output 2: bfloat16 [4, 896, 2560], P('rep', 'dp'), parts along dimension 0
- output 3: bfloat16 [4, 896, 2560], P('rep', 'dp'), parts along dimension 0
- output 4: bfloat16 [4, 2560, 896], P('rep', 'dp'), parts along dimension 0
There are 2 independent parts. The reference program is written for one: setup_inputs(seed, part) draws one part's arguments, and reference() takes and returns one part's arrays. A program takes and returns all parts, laid end to end along the dimension named above; an argument that names none is the same for every part.
All inputs are finite; a program needn't handle non-finite values.
Results may differ from the reference program's by a relative error of at most 0.018.
Values are sent between devices in bfloat16 or wider.
A program may use at most 1.5 GiB of HBM per device.

```python
import jax
import jax.numpy as jnp
from jax import lax

SEQUENCES = 64
TOKENS = 2048
D = 896
FF = 2560
LAYERS = 2
NAMES = ("w_gate", "w_up", "w_down")
SHAPES = {"w_gate": (LAYERS, D, FF), "w_up": (LAYERS, D, FF), "w_down": (LAYERS, FF, D)}


def bump(key, n, height):
    away = (jnp.arange(n, dtype=jnp.int32) - jax.random.randint(key, (), 0, n, jnp.int32)) % n
    return jnp.where(away < n // 8, height, 1.0)


def together(key, own, strength):
    shared = jax.random.normal(key, own.shape[1:], jnp.float32)
    return (own + strength * shared) * lax.rsqrt(1 + strength * strength)


def setup_inputs(seed: int = 0, part: int = 0) -> dict:
    kx, kdy, ka, kb, kz, kf, kh, kl, *kw = jax.random.split(jax.random.key(seed), 8 + len(NAMES))
    kx, kdy, ka, kb = (jax.random.fold_in(k, part) for k in (kx, kdy, ka, kb))
    shape = (SEQUENCES, TOKENS, D)
    much_x, much_dy = jax.random.uniform(kz, (2,), jnp.float32, 0.0, 1.0)
    layers = 2.0 ** jax.random.uniform(kl, (LAYERS, 1, 1), jnp.float32, -1.0, 1.0)
    x = together(ka, jax.random.normal(kx, shape, jnp.float32), much_x) * bump(kf, D, 4.0)
    dy = together(kb, jax.random.normal(kdy, shape, jnp.float32), much_dy)
    drawn = {"x": x.astype(jnp.bfloat16), "dy": (dy * (SEQUENCES * TOKENS) ** -0.5).astype(jnp.bfloat16)}
    for key, name in zip(kw, NAMES, strict=True):
        w = jax.random.normal(key, SHAPES[name], jnp.float32) * SHAPES[name][1] ** -0.5
        drawn[name] = (w * {"w_gate": 1.0, "w_up": bump(kh, FF, 4.0), "w_down": layers}[name]).astype(jnp.bfloat16)
    return drawn


def matmul(a, w):
    return jnp.dot(a, w, preferred_element_type=jnp.float32).astype(jnp.bfloat16)


def normed(h):
    wide = h.astype(jnp.float32)
    scale = lax.rsqrt(jnp.mean(wide**2, -1, keepdims=True) + 1e-6)
    return (wide * scale).astype(jnp.bfloat16)


def layer(h, w):
    a = normed(h)
    gate = jnp.dot(a, w["w_gate"], preferred_element_type=jnp.float32)
    up = jnp.dot(a, w["w_up"], preferred_element_type=jnp.float32)
    return h + matmul((jax.nn.silu(gate) * up).astype(jnp.bfloat16), w["w_down"])


def stack(weights, h):
    return lax.scan(lambda h, w: (layer(h, w), None), h, weights)[0]


def reference(x, dy, w_gate, w_up, w_down):
    weights = dict(zip(NAMES, (w_gate, w_up, w_down), strict=True))

    def take(so_far, sequence):
        h, by_y = sequence
        _, back = jax.vjp(stack, weights, h)
        by_weights, by_h = back(by_y)
        return jax.tree.map(lambda total, term: total + term.astype(jnp.float32), so_far, by_weights), by_h

    none_yet = {name: jnp.zeros(w.shape, jnp.float32) for name, w in weights.items()}
    by_weights, by_x = lax.scan(take, none_yet, (x, dy))
    return (by_x, *(by_weights[name].astype(jnp.bfloat16) for name in NAMES))
```

```python
import functools

import jax
import jax.numpy as jnp
from jax import lax
from jax.experimental import pallas as pl
from jax.experimental.pallas import tpu as pltpu
from jax.sharding import PartitionSpec as P

MESH = pl.DeviceIdType.MESH
BF, F32 = jnp.bfloat16, jnp.float32
D, FF, LAYERS = 896, 2560, 2
X, Y, Z = 0, 1, 2
GATE, UP, DOWN = 0, 1, 2


def place():
    me = lax.axis_index("dp")
    return lax.axis_index("rep"), (me // 16, (me // 4) % 4, me % 4)


def moved(core, at, dim, by):
    to = [(v + by) % 4 if d == dim else v for d, v in enumerate(at)]
    return core, to[0] * 16 + to[1] * 4 + to[2]


def meet(devices):
    barrier = pltpu.get_barrier_semaphore()
    for device in devices:
        pl.semaphore_signal(barrier, inc=1, device_id=device, device_id_type=MESH)
    pl.semaphore_wait(barrier, len(devices))


GATHER_ORDER = {GATE: (Y, X), UP: (X, Y), DOWN: (X, Y, Z)}
WINDOW = {GATE: (1280, 1280), UP: (1280, 1280), DOWN: (384, 512)}
SHARED = {GATE: (1280, 1280), UP: (1280, 1280), DOWN: (512, 384)}


def gather_kernel(gate, up, down, *refs):
    outs = [refs[0:3], refs[3:6]]
    zb, block, zs, zr, ms, mr, ds, dr, ls = refs[6:]
    core, at = place()
    given = (gate, up, down)
    partner = (1 - core, lax.axis_index("dp"))
    sends = []

    def columns(table, kind, of, part=None):
        step, width = table[kind]
        start = of * step
        if part is not None:
            width //= 2
            start = start + part * width
        return pl.ds(pl.multiple_of(start, 128), width)

    def view(l, kind, p, v, cols):
        order = GATHER_ORDER[kind]
        index = []
        for d in range(3 if kind == DOWN else 2):
            if d in order[:p]:
                index.append(slice(None))
            elif d == order[p]:
                index.append(v)
            else:
                index.append(at[d])
        return outs[l][kind].at[(*index, slice(None), cols)]

    def own(l, kind):
        cols = columns(WINDOW, kind, core)
        return down.at[l, :, cols] if kind == DOWN else block.at[l, kind]

    def send(src, dst, s, r, device):
        copy = pltpu.make_async_remote_copy(src, dst, s, r, device_id=device, device_id_type=MESH)
        copy.start()
        sends.append(copy)

    def arrived(ref, s, r):
        pltpu.make_async_remote_copy(ref, ref, s, r, device_id=partner, device_id_type=MESH).wait_recv()

    def first(l, kind, p):
        dim = GATHER_ORDER[kind][p]
        dst = view(l, kind, p, at[dim], columns(WINDOW, kind, core))
        src = own(l, kind) if p == 0 else dst
        for n, by in enumerate((1, -1)):
            send(src, dst, ms.at[l, kind, p, n], mr.at[l, kind, p, n], moved(core, at, dim, by))

    def relay(l, kind, p):
        dim = GATHER_ORDER[kind][p]
        for n, by in enumerate((1, -1)):
            v = (at[dim] - by) % 4
            arrived(view(l, kind, p, v, columns(WINDOW, kind, core)), ms.at[l, kind, p, n], mr.at[l, kind, p, n])
            half = view(l, kind, p, v, columns(WINDOW, kind, core, n))
            send(half, half, ms.at[l, kind, p, 2 + n], mr.at[l, kind, p, 2 + n], moved(core, at, dim, by))

    def last(l, kind, p):
        v = (at[GATHER_ORDER[kind][p]] + 2) % 4
        for n in range(2):
            half = view(l, kind, p, v, columns(WINDOW, kind, core, n))
            arrived(half, ms.at[l, kind, p, 2 + n], mr.at[l, kind, p, 2 + n])

    def share(l, kind, which, by):
        p = len(GATHER_ORDER[kind]) - 1
        v = (at[GATHER_ORDER[kind][p]] + by) % 4
        ref = view(l, kind, p, v, columns(SHARED, kind, core))
        send(ref, ref, ds.at[l, kind, which], dr.at[l, kind, which], partner)

    def keep(l, kind):
        return pltpu.make_async_copy(
            own(l, kind), view(l, kind, 0, at[GATHER_ORDER[kind][0]], columns(WINDOW, kind, core)), ls.at[l, kind]
        )

    meet([moved(core, at, d, by) for d in (X, Y, Z) for by in (1, 2, -1) if by != 2 or d == Z] + [partner])
    layers = range(LAYERS)
    for l in layers:
        for kind in (GATE, UP):
            cols = columns(WINDOW, kind, core)
            for by in (1, 3, 2):
                send(
                    given[kind].at[l, :, cols],
                    zb.at[l, kind, by - 1],
                    zs.at[l, kind, by - 1],
                    zr.at[l, kind, by - 1],
                    moved(core, at, Z, by),
                )
        first(l, DOWN, 0)
        keep(l, DOWN).start()
    for l in layers:
        for kind in (GATE, UP):
            for n in range(3):
                arrived(zb.at[l, kind, n], zs.at[l, kind, n], zr.at[l, kind, n])
            mine = given[kind][l, :, columns(WINDOW, kind, core)].astype(F32)
            come = [mine, *(zb[l, kind, n].astype(F32) for n in range(3))]
            for z in range(4):

                @pl.when(at[Z] == z)
                def _(z=z, come=come, kind=kind):
                    block[l, kind] = jnp.concatenate([come[(z - row) % 4] for row in range(4)], axis=0).astype(BF)

            first(l, kind, 0)
            keep(l, kind).start()
        relay(l, DOWN, 0)
    for l in layers:
        for kind in (GATE, UP):
            relay(l, kind, 0)
        last(l, DOWN, 0)
        keep(l, DOWN).wait()
        first(l, DOWN, 1)
    for l in layers:
        for kind in (GATE, UP):
            last(l, kind, 0)
            keep(l, kind).wait()
            first(l, kind, 1)
            share(l, kind, 0, 0)
        relay(l, DOWN, 1)
    for l in layers:
        last(l, DOWN, 1)
        first(l, DOWN, 2)
        share(l, DOWN, 0, 0)
        for kind in (GATE, UP):
            relay(l, kind, 1)
            share(l, kind, 1, 1)
            share(l, kind, 2, 3)
    for l in layers:
        for kind in (GATE, UP):
            last(l, kind, 1)
            share(l, kind, 3, 2)
        relay(l, DOWN, 2)
        share(l, DOWN, 1, 1)
        share(l, DOWN, 2, 3)
    for l in layers:
        last(l, DOWN, 2)
        share(l, DOWN, 3, 2)
    for l in layers:
        for kind in (GATE, UP, DOWN):
            p = len(GATHER_ORDER[kind]) - 1
            for which, by in enumerate((0, 1, 3, 2)):
                v = (at[GATHER_ORDER[kind][p]] + by) % 4
                ref = view(l, kind, p, v, columns(SHARED, kind, 1 - core))
                arrived(ref, ds.at[l, kind, which], dr.at[l, kind, which])
    for copy in sends:
        copy.wait_send()


def gather(w_gate, w_up, w_down):
    vmem, anywhere = pl.BlockSpec(memory_space=pltpu.VMEM), pl.BlockSpec(memory_space=pl.ANY)
    wide = jax.ShapeDtypeStruct((4, 4, D // 16, FF), BF)
    tall = jax.ShapeDtypeStruct((4, 4, 4, FF // 64, D), BF)
    dma = pltpu.SemaphoreType.DMA
    outs = pl.pallas_call(
        gather_kernel,
        name="gather",
        out_shape=(wide, wide, tall) * LAYERS,
        in_specs=[vmem] * 3,
        out_specs=(anywhere,) * (3 * LAYERS),
        scratch_shapes=[
            pltpu.VMEM((LAYERS, 2, 3, D // 64, FF // 2), BF),
            pltpu.VMEM((LAYERS, 2, D // 16, FF // 2), BF),
            dma((LAYERS, 2, 3)),
            dma((LAYERS, 2, 3)),
            dma((LAYERS, 3, 3, 4)),
            dma((LAYERS, 3, 3, 4)),
            dma((LAYERS, 3, 4)),
            dma((LAYERS, 3, 4)),
            dma((LAYERS, 3)),
        ],
        compiler_params=pltpu.CompilerParams(collective_id=0, has_side_effects=True),
    )(w_gate, w_up, w_down)
    return [
        (outs[3 * l].reshape(D, FF), outs[3 * l + 1].reshape(D, FF), outs[3 * l + 2].reshape(FF, D))
        for l in range(LAYERS)
    ]


SCATTER_ORDER = {GATE: (X, Y, Z), UP: (Y, X, Z), DOWN: (Z, X, Y)}
SPLIT = {GATE: 1280, UP: 1280, DOWN: 512}
COLS = {GATE: FF, UP: FF, DOWN: D}
STEP = {GATE: 256, UP: 256, DOWN: 128}
BLOCKS = {
    GATE: ((4, 56), (1, 56), (1, 16)),
    UP: ((4, 56), (1, 56), (1, 16)),
    DOWN: ((16, 40), (4, 40), (1, 40)),
}


def scatter_kernel(t_gate, t_up, t_down, o_gate, o_up, o_down, *refs):
    terms, outs = (t_gate, t_up, t_down), (o_gate, o_up, o_down)
    n_buf = 6
    buf = {(k, p): refs[(3 * k + p) * n_buf : (3 * k + p + 1) * n_buf] for k in range(3) for p in range(3)}
    refs = refs[9 * n_buf :]
    wide = {(k, p): refs[2 * k + p - 1] for k in range(3) for p in (1, 2)}
    stage = {(k, p): refs[6 + 2 * k + p - 1] for k in range(3) for p in (1, 2)}
    half = refs[12:14]
    ss, rs = refs[14:16]
    core, at = place()
    sends = []

    def leaving(k, p, v):
        if p == 0:
            if k == GATE:
                return terms[k].at[v]
            if k == UP:
                return terms[k].at[:, v]
            return terms[k].at[:, v]
        return stage[k, p].at[v]

    def held(k, p, v):
        return leaving(k, p, v) if p == 0 else wide[k, p].at[v]

    def part(k, n):
        return pl.ds(0, SPLIT[k]) if n == 0 else pl.ds(SPLIT[k], COLS[k] - SPLIT[k])

    def send(k, p, n, src, dst, by):
        copy = pltpu.make_async_remote_copy(
            src,
            dst,
            ss.at[k, p, n],
            rs.at[k, p, n],
            device_id=moved(core, at, SCATTER_ORDER[k][p], by),
            device_id_type=MESH,
        )
        copy.start()
        sends.append(copy)
        return copy

    def each(k, p, start, width, step):
        def over(body):
            lead = BLOCKS[k][p][0]
            n = width // STEP[k]

            def one(i, carry):
                body(i // n, pl.ds(pl.multiple_of(start + (i % n) * STEP[k], 128), STEP[k]), pl.ds(pl.multiple_of((i % n) * STEP[k], 128), STEP[k]))
                return carry

            lax.fori_loop(0, lead * n, one, 0)

        return over

    transit = {}

    def begin(k, p):
        v = at[SCATTER_ORDER[k][p]]
        from_left, from_right, sum_right, sum_left, left, right = buf[k, p]
        far = leaving(k, p, (v + 2) % 4)
        transit[k, p, 0] = send(k, p, 0, far.at[:, :, part(k, 0)], from_left, 1)
        transit[k, p, 1] = send(k, p, 1, far.at[:, :, part(k, 1)], from_right, -1)
        transit[k, p, 2] = send(
            k, p, 2, leaving(k, p, (v + 1) % 4).at[:, :, part(k, 1)], left.at[:, :, part(k, 1)], 1
        )
        transit[k, p, 3] = send(
            k, p, 3, leaving(k, p, (v + 3) % 4).at[:, :, part(k, 0)], right.at[:, :, part(k, 0)], -1
        )

    def middle(k, p):
        v = at[SCATTER_ORDER[k][p]]
        from_left, from_right, sum_right, sum_left, left, right = buf[k, p]
        for n, by, come, total, dst in ((0, 1, from_left, sum_right, left), (1, -1, from_right, sum_left, right)):
            transit[k, p, n].wait_recv()
            mine = held(k, p, (v + by) % 4)
            start, width = (0, SPLIT[k]) if n == 0 else (SPLIT[k], COLS[k] - SPLIT[k])

            @each(k, p, start, width, None)
            def _(i, whole, here, mine=mine, come=come, total=total):
                total[i, :, here] = (mine[i, :, whole].astype(F32) + come[i, :, here].astype(F32)).astype(BF)

            transit[k, p, 4 + n] = send(k, p, 4 + n, total, dst.at[:, :, part(k, n)], by)

    def end(k, p):
        v = at[SCATTER_ORDER[k][p]]
        left, right = buf[k, p][4:]
        for n in range(2, 6):
            transit[k, p, n].wait_recv()
        mine = held(k, p, v)

        @each(k, p, 0, COLS[k], None)
        def _(i, cols, _):
            total = mine[i, :, cols].astype(F32) + left[i, :, cols].astype(F32) + right[i, :, cols].astype(F32)
            if p == 2:
                if k == DOWN:
                    outs[k][:, cols] = total.astype(BF)
                else:
                    outs[k][:, cols] = total[:14].astype(BF)
            elif k != DOWN and p == 1:
                for z in range(4):
                    rows = jnp.concatenate([total[14 * z : 14 * z + 14], jnp.zeros((2, STEP[k]), F32)], axis=0)
                    wide[k, 2][z, 0, :, cols] = rows
                    stage[k, 2][z, 0, :, cols] = rows.astype(BF)
            elif k != DOWN or p == 1:
                wide[k, p + 1][i, 0, :, cols] = total
                stage[k, p + 1][i, 0, :, cols] = total.astype(BF)
            else:
                wide[k, 1][i // 4, i % 4, :, cols] = total
                stage[k, 1][i // 4, i % 4, :, cols] = total.astype(BF)

    meet([moved(core, at, d, by) for d in (X, Y, Z) for by in (1, -1)])
    kinds = (DOWN, GATE, UP)
    for k in kinds:
        begin(k, 0)
    for p in range(3):
        for k in kinds:
            middle(k, p)
        for k in kinds:
            end(k, p)
            if p < 2:
                begin(k, p + 1)
    for copy in sends:
        copy.wait_send()


def scatter(t_gate, t_up, t_down, number):
    vmem = pl.BlockSpec(memory_space=pltpu.VMEM)
    scratch = []
    for k in range(3):
        for lead, rows in BLOCKS[k]:
            one, other = SPLIT[k], COLS[k] - SPLIT[k]
            for cols in (one, other, one, other, COLS[k], COLS[k]):
                scratch.append(pltpu.VMEM((lead, rows, cols), BF))
    for kind in (F32, BF):
        for k in range(3):
            for lead, rows in BLOCKS[k][1:]:
                scratch.append(pltpu.VMEM((4, lead, rows, COLS[k]), kind))
    scratch += [pltpu.VMEM((8, 128), BF)] * 2
    scratch += [pltpu.SemaphoreType.DMA((3, 3, 6))] * 2
    return pl.pallas_call(
        scatter_kernel,
        name=f"scatter_{number}",
        out_shape=(
            jax.ShapeDtypeStruct((D // 64, FF), BF),
            jax.ShapeDtypeStruct((D // 64, FF), BF),
            jax.ShapeDtypeStruct((FF // 64, D), BF),
        ),
        in_specs=[vmem] * 3,
        out_specs=(vmem,) * 3,
        scratch_shapes=scratch,
        compiler_params=pltpu.CompilerParams(
            collective_id=1, has_side_effects=True, vmem_limit_bytes=60 * 1024 * 1024
        ),
    )(t_gate.reshape(4, 4, 56, FF), t_up.reshape(4, 4, 56, FF), t_down.reshape(16, 4, 40, D))


def dot(a, b, over=((1,), (0,))):
    return lax.dot_general(a, b, (over, ((), ())), preferred_element_type=F32)


def norm(h):
    wide = h.astype(F32)
    scale = lax.rsqrt(jnp.mean(wide**2, -1, keepdims=True) + 1e-6)
    return (wide * scale).astype(BF), scale


def norm_back(h, scale, by_a):
    wide, by = h.astype(F32), by_a.astype(F32)
    inner = jnp.mean(by * wide, -1, keepdims=True)
    return (by * scale - wide * (scale * scale * scale * inner)).astype(BF)


def gated(gate, up):
    return (jax.nn.silu(gate) * up).astype(BF)


def back(h, a, scale, gate, up, act, by_y, weights):
    w_gate, w_up, w_down = weights
    by_act = dot(by_y, w_down, ((1,), (1,))).astype(BF)
    t_down = dot(act, by_y, ((0,), (0,))).astype(BF)
    sig = jax.nn.sigmoid(gate)
    by_act = by_act.astype(F32)
    by_up = (by_act * (gate * sig)).astype(BF)
    by_gate = (by_act * up * (sig * (1 + gate * (1 - sig)))).astype(BF)
    t_gate = dot(a, by_gate, ((0,), (0,))).astype(BF)
    t_up = dot(a, by_up, ((0,), (0,))).astype(BF)
    by_a = dot(by_gate, w_gate, ((1,), (1,))).astype(BF) + dot(by_up, w_up, ((1,), (1,))).astype(BF)
    return by_y + norm_back(h, scale, by_a), (t_gate, t_up, t_down)


def local(x, dy, w_gate, w_up, w_down):
    x, dy = x[0], dy[0]
    first, second = gather(w_gate, w_up, w_down)
    a0, s0 = norm(x)
    g0, u0 = dot(a0, first[0]), dot(a0, first[1])
    act0 = gated(g0, u0)
    h = x + dot(act0, first[2]).astype(BF)
    a1, s1 = norm(h)
    g1, u1 = dot(a1, second[0]), dot(a1, second[1])
    by_h, terms = back(h, a1, s1, g1, u1, gated(g1, u1), dy, second)
    of_second = scatter(*terms, 1)
    by_x, terms = back(x, a0, s0, g0, u0, act0, by_h, first)
    of_first = scatter(*terms, 0)
    return (by_x[None], *(jnp.stack(pair) for pair in zip(of_first, of_second)))


def solution(mesh):
    tokens, rows = P(("rep", "dp")), P(None, "dp", None)
    return jax.shard_map(
        local,
        mesh=mesh,
        in_specs=(tokens, tokens, rows, rows, rows),
        out_specs=(tokens, *([P("rep", "dp", None)] * 3)),
        check_vma=False,
    )
```

```python
import functools

import jax
import jax.numpy as jnp
from jax import lax
from jax.experimental import pallas as pl
from jax.experimental.pallas import tpu as pltpu
from jax.sharding import PartitionSpec as P

MESH = pl.DeviceIdType.MESH
BF, F32 = jnp.bfloat16, jnp.float32
D, FF, LAYERS = 896, 2560, 2
X, Y, Z = 0, 1, 2
GATE, UP, DOWN = 0, 1, 2


def place():
    me = lax.axis_index("dp")
    return lax.axis_index("rep"), (me // 16, (me // 4) % 4, me % 4)


def moved(core, at, dim, by):
    to = [(v + by) % 4 if d == dim else v for d, v in enumerate(at)]
    return core, to[0] * 16 + to[1] * 4 + to[2]


def meet(devices):
    barrier = pltpu.get_barrier_semaphore()
    for device in devices:
        pl.semaphore_signal(barrier, inc=1, device_id=device, device_id_type=MESH)
    pl.semaphore_wait(barrier, len(devices))


BYTES = 63 * 1024 * 1024
GATHER_ORDER = {GATE: (Y, X), UP: (X, Y), DOWN: (X, Y, Z)}
WINDOW = {GATE: (1280, 1280), UP: (1280, 1280), DOWN: (384, 512)}
SHARED = {GATE: (1280, 1280), UP: (1280, 1280), DOWN: (512, 384)}


def gather_plan(l, given, outs, refs):
    zb, block, zs, zr, ms, mr, ds, dr, ls = refs
    core, at = place()
    partner = (1 - core, lax.axis_index("dp"))

    def columns(table, kind, of, part=None):
        step, width = table[kind]
        start = of * step
        if part is not None:
            width //= 2
            start = start + part * width
        return pl.ds(pl.multiple_of(start, 128), width)

    def view(kind, p, by, cols):
        order = GATHER_ORDER[kind]
        index = []
        for d in range(3 if kind == DOWN else 2):
            if d in order[:p]:
                index.append(slice(None))
            elif d == order[p]:
                index.append((at[d] + by) % 4)
            else:
                index.append(at[d])
        return outs[kind].at[(*index, slice(None), cols)]

    def mine(kind):
        cols = columns(WINDOW, kind, core)
        return given[kind].at[l, :, cols] if kind == DOWN else block.at[kind]

    def remote(src, dst, s, r, device):
        return pltpu.make_async_remote_copy(src, dst, s, r, device_id=device, device_id_type=MESH)

    def near(kind, by):
        src, sem = given[kind].at[l, :, columns(WINDOW, kind, core)], (kind, by - 1)
        return remote(src, zb.at[sem], zs.at[sem], zr.at[sem], moved(core, at, Z, by))

    def first(kind, p, n):
        dst = view(kind, p, 0, columns(WINDOW, kind, core))
        to = moved(core, at, GATHER_ORDER[kind][p], (1, -1)[n])
        return remote(mine(kind) if p == 0 else dst, dst, ms.at[kind, p, n], mr.at[kind, p, n], to)

    def relay(kind, p, n):
        by = (1, -1)[n]
        half = view(kind, p, -by, columns(WINDOW, kind, core, n))
        to = moved(core, at, GATHER_ORDER[kind][p], by)
        return remote(half, half, ms.at[kind, p, 2 + n], mr.at[kind, p, 2 + n], to)

    SHARES = (0, 1, 3, 2)

    def share(kind, which):
        ref = view(kind, len(GATHER_ORDER[kind]) - 1, SHARES[which], columns(SHARED, kind, core))
        return remote(ref, ref, ds.at[kind, which], dr.at[kind, which], partner)

    def keep(kind):
        return pltpu.make_async_copy(mine(kind), view(kind, 0, 0, columns(WINDOW, kind, core)), ls.at[kind])

    def arrived(ref, s, r):
        remote(ref, ref, s, r, partner).wait_recv()

    def start_first(kind, p):
        for n in range(2):
            first(kind, p, n).start()

    def pass_on(kind, p):
        for n in range(2):
            ref = view(kind, p, -(1, -1)[n], columns(WINDOW, kind, core))
            arrived(ref, ms.at[kind, p, n], mr.at[kind, p, n])
            relay(kind, p, n).start()

    def finish(kind, p):
        for n in range(2):
            arrived(view(kind, p, 2, columns(WINDOW, kind, core, n)), ms.at[kind, p, 2 + n], mr.at[kind, p, 2 + n])

    def stage0():
        meet([moved(core, at, d, by) for d in (X, Y, Z) for by in (1, 2, -1) if by != 2 or d == Z] + [partner])
        for kind in (GATE, UP):
            for by in (1, 3, 2):
                near(kind, by).start()
        start_first(DOWN, 0)
        keep(DOWN).start()

    def stage1():
        for kind in (GATE, UP):
            for n in range(3):
                arrived(zb.at[kind, n], zs.at[kind, n], zr.at[kind, n])
            come = [given[kind][l, :, columns(WINDOW, kind, core)].astype(F32)]
            come += [zb[kind, n].astype(F32) for n in range(3)]
            for z in range(4):

                @pl.when(at[Z] == z)
                def _(z=z, come=come, kind=kind):
                    block[kind] = jnp.concatenate([come[(z - row) % 4] for row in range(4)], axis=0).astype(BF)

            start_first(kind, 0)
            keep(kind).start()
        pass_on(DOWN, 0)

    def stage2():
        for kind in (GATE, UP):
            pass_on(kind, 0)
        finish(DOWN, 0)
        keep(DOWN).wait()
        start_first(DOWN, 1)

    def stage3():
        for kind in (GATE, UP):
            finish(kind, 0)
            keep(kind).wait()
            start_first(kind, 1)
            share(kind, 0).start()
        pass_on(DOWN, 1)

    def stage4():
        finish(DOWN, 1)
        start_first(DOWN, 2)
        share(DOWN, 0).start()

    def stage5():
        for kind in (GATE, UP):
            pass_on(kind, 1)
            share(kind, 1).start()
            share(kind, 2).start()

    def stage6():
        pass_on(DOWN, 2)
        share(DOWN, 1).start()
        share(DOWN, 2).start()

    def stage7():
        for kind in (GATE, UP):
            finish(kind, 1)
            share(kind, 3).start()

    def stage8():
        finish(DOWN, 2)
        share(DOWN, 3).start()
        for kind in (GATE, UP, DOWN):
            for which in range(4):
                p = len(GATHER_ORDER[kind]) - 1
                ref = view(kind, p, SHARES[which], columns(SHARED, kind, 1 - core))
                arrived(ref, ds.at[kind, which], dr.at[kind, which])
        for kind in (GATE, UP):
            for by in (1, 3, 2):
                near(kind, by).wait_send()
        for kind in (GATE, UP, DOWN):
            for p in range(len(GATHER_ORDER[kind])):
                for n in range(2):
                    first(kind, p, n).wait_send()
                    relay(kind, p, n).wait_send()
            for which in range(4):
                share(kind, which).wait_send()

    return [stage0, stage1, stage2, stage3, stage4, stage5, stage6, stage7, stage8]


def gather_scratch():
    dma = pltpu.SemaphoreType.DMA
    return [
        pltpu.VMEM((2, 3, D // 64, FF // 2), BF),
        pltpu.VMEM((2, D // 16, FF // 2), BF),
        dma((2, 3)),
        dma((2, 3)),
        dma((3, 3, 4)),
        dma((3, 3, 4)),
        dma((3, 4)),
        dma((3, 4)),
        dma((3,)),
    ]


VMEM, ANYWHERE = pl.BlockSpec(memory_space=pltpu.VMEM), pl.BlockSpec(memory_space=pl.ANY)


def gathered():
    wide = jax.ShapeDtypeStruct((4, 4, D // 16, FF), BF)
    return wide, wide, jax.ShapeDtypeStruct((4, 4, 4, FF // 64, D), BF)


def matrices(gate, up, down):
    return gate.reshape(D, FF), up.reshape(D, FF), down.reshape(FF, D)


def gather(shards):
    def kernel(*refs):
        for stage in gather_plan(0, refs[:3], refs[3:6], refs[6:]):
            stage()

    return matrices(
        *pl.pallas_call(
            kernel,
            name="gather",
            out_shape=gathered(),
            in_specs=[VMEM] * 3,
            out_specs=(ANYWHERE,) * 3,
            scratch_shapes=gather_scratch(),
            compiler_params=pltpu.CompilerParams(collective_id=0, has_side_effects=True),
        )(*shards)
    )


SCATTER_ORDER = {GATE: (X, Y, Z), UP: (Y, X, Z), DOWN: (Z, X, Y)}
SPLIT = {GATE: 1280, UP: 1280, DOWN: 512}
COLS = {GATE: FF, UP: FF, DOWN: D}
STEP = {GATE: 256, UP: 256, DOWN: 128}
BLOCKS = {
    GATE: ((4, 56), (1, 56), (1, 16)),
    UP: ((4, 56), (1, 56), (1, 16)),
    DOWN: ((16, 40), (4, 40), (1, 40)),
}
KINDS = (DOWN, GATE, UP)


def scatter_plan(terms, outs, refs):
    refs = list(refs)
    buf = {(k, p): [refs.pop(0) for _ in range(4)] for k in range(3) for p in range(3)}
    wide = {(k, p): refs.pop(0) for k in range(3) for p in (1, 2)}
    stage = {(k, p): refs.pop(0) for k in range(3) for p in (1, 2)}
    own = {k: [refs.pop(0) for _ in range(3)] for k in range(3)}
    ss, rs, ls = refs
    core, at = place()

    def block(k, p, by):
        v = (at[SCATTER_ORDER[k][p]] + by) % 4
        if p:
            return stage[k, p].at[v]
        return terms[k].at[v] if k == GATE else terms[k].at[:, v]

    def part(k, n):
        return pl.ds(0, SPLIT[k]) if n == 0 else pl.ds(SPLIT[k], COLS[k] - SPLIT[k])

    def flow(k, p, n):
        from_left, from_right, left, right = buf[k, p]
        src, dst = {
            0: lambda: (block(k, p, 2).at[:, :, part(k, 0)], from_left),
            1: lambda: (block(k, p, 2).at[:, :, part(k, 1)], from_right),
            2: lambda: (block(k, p, 1).at[:, :, part(k, 1)], left.at[:, :, part(k, 1)]),
            3: lambda: (block(k, p, -1).at[:, :, part(k, 0)], right.at[:, :, part(k, 0)]),
            4: lambda: (from_left, left.at[:, :, part(k, 0)]),
            5: lambda: (from_right, right.at[:, :, part(k, 1)]),
        }[n]()
        to = moved(core, at, SCATTER_ORDER[k][p], (1, -1)[n % 2])
        sems = ss.at[k, p, n], rs.at[k, p, n]
        return pltpu.make_async_remote_copy(src, dst, *sems, device_id=to, device_id_type=MESH)

    def load(k, n):
        src = (lambda: block(k, 0, 1).at[:, :, part(k, 0)], lambda: block(k, 0, -1).at[:, :, part(k, 1)], lambda: block(k, 0, 0))[n]()
        return pltpu.make_async_copy(src, own[k][n], ls.at[k, n])

    def each(k, p, width, body):
        count = width // STEP[k]

        def one(i, carry):
            body(i // count, (i % count) * STEP[k])
            return carry

        lax.fori_loop(0, BLOCKS[k][p][0] * count, one, 0)

    def here(k, start):
        return pl.ds(pl.multiple_of(start, 128), STEP[k])

    def begin(k, p):
        for n in range(4):
            flow(k, p, n).start()
        if p == 0:
            for n in range(3):
                load(k, n).start()

    def middle(k, p):
        for n in range(2):
            flow(k, p, n).wait_recv()
            if p == 0:
                load(k, n).wait()
            come, before = buf[k, p][n], 0 if p == 0 or n == 0 else SPLIT[k]
            mine = own[k][n] if p == 0 else wide[k, p].at[(at[SCATTER_ORDER[k][p]] + (1, -1)[n]) % 4]

            def add(i, start, mine=mine, come=come, before=before):
                cols = here(k, start)
                come[i, :, cols] = (mine[i, :, here(k, start + before)].astype(F32) + come[i, :, cols].astype(F32)).astype(BF)

            each(k, p, SPLIT[k] if n == 0 else COLS[k] - SPLIT[k], add)
            flow(k, p, 4 + n).start()

    def end(k, p):
        left, right = buf[k, p][2:]
        for n in range(2, 6):
            flow(k, p, n).wait_recv()
        if p == 0:
            load(k, 2).wait()
        mine = own[k][2] if p == 0 else wide[k, p].at[at[SCATTER_ORDER[k][p]]]

        def add(i, start):
            cols = here(k, start)
            total = mine[i, :, cols].astype(F32) + left[i, :, cols].astype(F32) + right[i, :, cols].astype(F32)
            if p == 2:
                outs[k][:, cols] = total[: outs[k].shape[0]].astype(BF)
            elif k != DOWN and p == 1:
                for z in range(4):
                    rows = jnp.concatenate([total[14 * z : 14 * z + 14], jnp.zeros((2, STEP[k]), F32)], axis=0)
                    wide[k, 2][z, 0, :, cols] = rows
                    stage[k, 2][z, 0, :, cols] = rows.astype(BF)
            else:
                at_row = (i, 0) if k != DOWN or p == 1 else (i // 4, i % 4)
                wide[k, p + 1][(*at_row, slice(None), cols)] = total
                stage[k, p + 1][(*at_row, slice(None), cols)] = total.astype(BF)

        each(k, p, COLS[k], add)
        if p < 2:
            begin(k, p + 1)

    def enter():
        meet([moved(core, at, d, by) for d in (X, Y, Z) for by in (1, -1)])
        for k in KINDS:
            begin(k, 0)

    def leave():
        for k in KINDS:
            for p in range(3):
                for n in range(6):
                    flow(k, p, n).wait_send()

    stages = [enter]
    for p in range(3):
        stages += [functools.partial(middle, k, p) for k in KINDS]
        stages += [functools.partial(end, k, p) for k in KINDS]
    return [*stages, leave]


def scatter_scratch():
    scratch = []
    for k in range(3):
        for lead, rows in BLOCKS[k]:
            for cols in (SPLIT[k], COLS[k] - SPLIT[k], COLS[k], COLS[k]):
                scratch.append(pltpu.VMEM((lead, rows, cols), BF))
    for kind in (F32, BF):
        for k in range(3):
            for lead, rows in BLOCKS[k][1:]:
                scratch.append(pltpu.VMEM((4, lead, rows, COLS[k]), kind))
    for k in range(3):
        lead, rows = BLOCKS[k][0]
        for cols in (SPLIT[k], COLS[k] - SPLIT[k], COLS[k]):
            scratch.append(pltpu.VMEM((lead, rows, cols), BF))
    dma = pltpu.SemaphoreType.DMA
    return [*scratch, dma((3, 3, 6)), dma((3, 3, 6)), dma((3, 3))]


def scattered():
    wide = jax.ShapeDtypeStruct((D // 64, FF), BF)
    return wide, wide, jax.ShapeDtypeStruct((FF // 64, D), BF)


def blocked(t_gate, t_up, t_down):
    return t_gate.reshape(4, 4, 56, FF), t_up.reshape(4, 4, 56, FF), t_down.reshape(16, 4, 40, D)


def scatter(terms):
    def kernel(*refs):
        for stage in scatter_plan(refs[:3], refs[3:6], refs[6:]):
            stage()

    return pl.pallas_call(
        kernel,
        name="scatter",
        out_shape=scattered(),
        in_specs=[ANYWHERE] * 3,
        out_specs=(VMEM,) * 3,
        scratch_shapes=scatter_scratch(),
        compiler_params=pltpu.CompilerParams(collective_id=1, has_side_effects=True, vmem_limit_bytes=BYTES),
    )(*blocked(*terms))


TOKENS, CHUNK = 2048, 512
GATHER_AT = ((0, 0), (0, 3), (1, 0), (1, 3), (2, 0), (3, 3), (4, 3), (6, 3), (7, 3))
SCATTER_AT = (
    (0, 0),
    *((1, 3), (2, 0), (2, 0)),
    *((4, 0), (4, 3), (5, 0)),
    *((5, 3), (5, 3), (5, 3)),
    *((6, 0), (6, 3), (6, 3)),
    *((7, 0), (7, 0), (7, 0)),
    *((7, 3), (7, 3), (7, 3)),
    (7, 5),
)


def run(stages, places, number):
    for stage, (tile, chunk) in zip(stages, places, strict=True):
        if chunk == number:
            pl.when(pl.program_id(0) == tile)(stage)

ROWS = ((1,), (1,))
FIRST = ((0,), (0,))


def dot(a, b, over=((1,), (0,))):
    return lax.dot_general(a, b, (over, ((), ())), preferred_element_type=F32)


def norm(h):
    wide = h.astype(F32)
    scale = lax.rsqrt(jnp.mean(wide * wide, -1, keepdims=True) + 1e-6)
    return (wide * scale).astype(BF), scale


def chunks():
    return [slice(j, j + CHUNK) for j in range(0, FF, CHUNK)]


def forward_kernel(h_ref, gate_ref, up_ref, down_ref, *refs):
    out_ref = refs[3]
    plan = gather_plan(1, refs[:3], refs[4:7], refs[7:])
    h = h_ref[...]
    a, _ = norm(h)
    total = None
    for number, cols in enumerate(chunks()):
        run(plan, GATHER_AT, number)
        gate, up = dot(a, gate_ref[:, cols]), dot(a, up_ref[:, cols])
        act = (gate * jax.nn.sigmoid(gate) * up).astype(BF)
        more = dot(act, down_ref[cols, :])
        total = more if total is None else total + more
    run(plan, GATHER_AT, len(chunks()))
    out_ref[...] = h + total.astype(BF)


def backward_kernel(hosts, h_ref, by_ref, gate_ref, up_ref, down_ref, *refs):
    if hosts:
        terms, refs = refs[:3], refs[3:]
    by_h_ref, a_ref, act_ref, by_gate_ref, by_up_ref, *refs = refs
    plan, places = (scatter_plan(terms, refs[:3], refs[3:]), SCATTER_AT) if hosts else ((), ())
    h, by = h_ref[...], by_ref[...]
    a, scale = norm(h)
    a_ref[...] = a
    total = None
    for number, cols in enumerate(chunks()):
        run(plan, places, number)
        gate, up = dot(a, gate_ref[:, cols]), dot(a, up_ref[:, cols])
        by_act = dot(by, down_ref[cols, :], ROWS).astype(BF).astype(F32)
        sig = jax.nn.sigmoid(gate)
        silu = gate * sig
        act_ref[:, cols] = (silu * up).astype(BF)
        by_up = (by_act * silu).astype(BF)
        by_gate = (by_act * up * (sig + silu * (1 - sig))).astype(BF)
        by_up_ref[:, cols] = by_up
        by_gate_ref[:, cols] = by_gate
        more = dot(by_gate, gate_ref[:, cols], ROWS) + dot(by_up, up_ref[:, cols], ROWS)
        total = more if total is None else total + more
    run(plan, places, len(chunks()))
    by_a = total.astype(BF).astype(F32)
    wide = h.astype(F32)
    inner = jnp.mean(by_a * wide, -1, keepdims=True)
    by_h_ref[...] = by + (by_a * scale - wide * (scale * scale * scale * inner)).astype(BF)


def weights_kernel(a_ref, by_ref, act_ref, by_gate_ref, by_up_ref, t_gate_ref, t_up_ref, t_down_ref, turned):
    @pl.when(pl.program_id(0) == 0)
    def _():
        turned[...] = a_ref[...].T

    t_down_ref[...] = dot(act_ref[...], by_ref[...], FIRST).astype(BF)
    t_gate_ref[...] = dot(turned[...], by_gate_ref[...]).astype(BF)
    t_up_ref[...] = dot(turned[...], by_up_ref[...]).astype(BF)


def whole(shape):
    return pl.BlockSpec(shape, lambda i: (0, 0), pipeline_mode=pl.Buffered(1))


def of_tokens(tile, cols):
    return pl.BlockSpec((tile, cols), lambda i: (i, 0))


def cost(matmuls):
    return pl.CostEstimate(flops=matmuls * 2 * TOKENS * D * FF, transcendentals=0, bytes_accessed=40_000_000)


def shaped(*shape):
    return jax.ShapeDtypeStruct(shape, BF)


BIG = pltpu.CompilerParams(vmem_limit_bytes=BYTES)
WEIGHTS = [whole((D, FF)), whole((D, FF)), whole((FF, D))]


def forward(h, weights, shards):
    tile = TOKENS // 8
    h, *others = pl.pallas_call(
        forward_kernel,
        name="forward",
        grid=(TOKENS // tile,),
        out_shape=(shaped(TOKENS, D), *gathered()),
        in_specs=[of_tokens(tile, D), *WEIGHTS, *[VMEM] * 3],
        out_specs=(of_tokens(tile, D), *[ANYWHERE] * 3),
        scratch_shapes=gather_scratch(),
        compiler_params=pltpu.CompilerParams(collective_id=2, has_side_effects=True, vmem_limit_bytes=BYTES),
        cost_estimate=cost(3),
    )(h, *weights, *shards)
    return h, matrices(*others)


def back(h, by, weights, number, terms=()):
    tile = TOKENS // 8 if terms else TOKENS // 4
    params = BIG
    if terms:
        params = pltpu.CompilerParams(collective_id=3, has_side_effects=True, vmem_limit_bytes=BYTES)
    by_h, a, act, by_gate, by_up, *sums = pl.pallas_call(
        functools.partial(backward_kernel, bool(terms)),
        name=f"backward_{number}",
        grid=(TOKENS // tile,),
        out_shape=(shaped(TOKENS, D), shaped(TOKENS, D), *[shaped(TOKENS, FF)] * 3, *(scattered() if terms else ())),
        in_specs=[of_tokens(tile, D), of_tokens(tile, D), *WEIGHTS, *([ANYWHERE] * len(terms))],
        out_specs=(
            *[of_tokens(tile, D)] * 2,
            *[of_tokens(tile, FF)] * 3,
            *([VMEM] * len(terms)),
        ),
        scratch_shapes=scatter_scratch() if terms else (),
        compiler_params=params,
        cost_estimate=cost(5),
    )(h, by, *weights, *(blocked(*terms) if terms else ()))
    side = pl.BlockSpec((TOKENS, CHUNK), lambda i: (0, i))
    terms = pl.pallas_call(
        weights_kernel,
        name=f"weights_{number}",
        grid=(FF // CHUNK,),
        out_shape=(shaped(D, FF), shaped(D, FF), shaped(FF, D)),
        in_specs=[whole((TOKENS, D)), whole((TOKENS, D)), side, side, side],
        out_specs=(
            pl.BlockSpec((D, CHUNK), lambda i: (0, i)),
            pl.BlockSpec((D, CHUNK), lambda i: (0, i)),
            pl.BlockSpec((CHUNK, D), lambda i: (i, 0)),
        ),
        scratch_shapes=[pltpu.VMEM((D, TOKENS), BF)],
        compiler_params=BIG,
        cost_estimate=cost(3),
    )(a, by, act, by_gate, by_up)
    return by_h, terms, sums


def local(x, dy, *shards):
    x, dy = x[0], dy[0]
    first = gather(shards)
    h, second = forward(x, first, shards)
    by_h, terms, _ = back(h, dy, second, 1)
    by_x, terms, of_second = back(x, by_h, first, 0, terms)
    of_first = scatter(terms)
    return (by_x[None], *(jnp.stack(pair) for pair in zip(of_first, of_second)))


def solution(mesh):
    tokens, rows = P(("rep", "dp")), P(None, "dp", None)
    return jax.shard_map(
        local,
        mesh=mesh,
        in_specs=(tokens, tokens, rows, rows, rows),
        out_specs=(tokens, *([P("rep", "dp", None)] * 3)),
        check_vma=False,
    )
```

```python
import functools

import jax
import jax.numpy as jnp
from jax import lax
from jax.experimental import pallas as pl
from jax.experimental.pallas import tpu as pltpu
from jax.sharding import PartitionSpec as P

MESH = pl.DeviceIdType.MESH
BF, F32 = jnp.bfloat16, jnp.float32
D, FF, LAYERS = 896, 2560, 2
X, Y, Z = 0, 1, 2
GATE, UP, DOWN = 0, 1, 2


def place():
    me = lax.axis_index("dp")
    return lax.axis_index("rep"), (me // 16, (me // 4) % 4, me % 4)


def moved(core, at, dim, by):
    to = [(v + by) % 4 if d == dim else v for d, v in enumerate(at)]
    return core, to[0] * 16 + to[1] * 4 + to[2]


def meet(devices):
    barrier = pltpu.get_barrier_semaphore()
    for device in devices:
        pl.semaphore_signal(barrier, inc=1, device_id=device, device_id_type=MESH)
    pl.semaphore_wait(barrier, len(devices))


BYTES = 63 * 1024 * 1024
GATHER_ORDER = {GATE: (Y, X), UP: (X, Y), DOWN: (X, Y, Z)}
WINDOW = {GATE: (1280, 1280), UP: (1280, 1280), DOWN: (384, 512)}
SHARED = {GATE: (1280, 1280), UP: (1280, 1280), DOWN: (512, 384)}


def gather_plan(l, given, outs, refs, meeting=True):
    zb, block, zs, zr, ms, mr, ds, dr, ls = refs
    core, at = place()
    partner = (1 - core, lax.axis_index("dp"))

    def columns(table, kind, of, part=None):
        step, width = table[kind]
        start = of * step
        if part is not None:
            width //= 2
            start = start + part * width
        return pl.ds(pl.multiple_of(start, 128), width)

    def view(kind, p, by, cols):
        order = GATHER_ORDER[kind]
        index = []
        for d in range(3 if kind == DOWN else 2):
            if d in order[:p]:
                index.append(slice(None))
            elif d == order[p]:
                index.append((at[d] + by) % 4)
            else:
                index.append(at[d])
        return outs[kind].at[(*index, slice(None), cols)]

    def mine(kind):
        cols = columns(WINDOW, kind, core)
        return given[kind].at[l, :, cols] if kind == DOWN else block.at[kind]

    def remote(src, dst, s, r, device):
        return pltpu.make_async_remote_copy(src, dst, s, r, device_id=device, device_id_type=MESH)

    def near(kind, by):
        src, sem = given[kind].at[l, :, columns(WINDOW, kind, core)], (kind, by - 1)
        return remote(src, zb.at[sem], zs.at[sem], zr.at[sem], moved(core, at, Z, by))

    def first(kind, p, n, part):
        dst = view(kind, p, 0, columns(WINDOW, kind, core, part))
        width = WINDOW[kind][1] // 2
        src = dst
        if p == 0 and kind == DOWN:
            src = given[kind].at[l, :, columns(WINDOW, kind, core, part)]
        elif p == 0:
            src = block.at[kind, :, pl.ds(part * width, width)]
        to = moved(core, at, GATHER_ORDER[kind][p], (1, -1)[n])
        which = n if part == n else 4 + n
        return remote(src, dst, ms.at[kind, p, which], mr.at[kind, p, which], to)

    def relay(kind, p, n):
        by = (1, -1)[n]
        half = view(kind, p, -by, columns(WINDOW, kind, core, n))
        to = moved(core, at, GATHER_ORDER[kind][p], by)
        return remote(half, half, ms.at[kind, p, 2 + n], mr.at[kind, p, 2 + n], to)

    SHARES = (0, 1, 3, 2)

    def share(kind, which):
        ref = view(kind, len(GATHER_ORDER[kind]) - 1, SHARES[which], columns(SHARED, kind, core))
        return remote(ref, ref, ds.at[kind, which], dr.at[kind, which], partner)

    def keep(kind):
        return pltpu.make_async_copy(mine(kind), view(kind, 0, 0, columns(WINDOW, kind, core)), ls.at[kind])

    def arrived(ref, s, r):
        remote(ref, ref, s, r, partner).wait_recv()

    def start_first(kind, p):
        for part in (0, 1):
            for n in range(2):
                first(kind, p, n, n if part == 0 else 1 - n).start()

    def pass_on(kind, p):
        for n in range(2):
            ref = view(kind, p, -(1, -1)[n], columns(WINDOW, kind, core, n))
            arrived(ref, ms.at[kind, p, n], mr.at[kind, p, n])
            relay(kind, p, n).start()

    def rest(kind, p):
        for n in range(2):
            ref = view(kind, p, -(1, -1)[n], columns(WINDOW, kind, core, 1 - n))
            arrived(ref, ms.at[kind, p, 4 + n], mr.at[kind, p, 4 + n])

    def finish(kind, p):
        for n in range(2):
            arrived(view(kind, p, 2, columns(WINDOW, kind, core, n)), ms.at[kind, p, 2 + n], mr.at[kind, p, 2 + n])

    def stage0():
        if meeting:
            meet([moved(core, at, d, by) for d in (X, Y, Z) for by in (1, 2, -1) if by != 2 or d == Z] + [partner])
        for kind in (GATE, UP):
            for by in (1, 3, 2):
                near(kind, by).start()
        start_first(DOWN, 0)
        keep(DOWN).start()

    def stage1():
        for kind in (GATE, UP):
            for n in range(3):
                arrived(zb.at[kind, n], zs.at[kind, n], zr.at[kind, n])
            come = [given[kind][l, :, columns(WINDOW, kind, core)].astype(F32)]
            come += [zb[kind, n].astype(F32) for n in range(3)]
            for z in range(4):

                @pl.when(at[Z] == z)
                def _(z=z, come=come, kind=kind):
                    block[kind] = jnp.concatenate([come[(z - row) % 4] for row in range(4)], axis=0).astype(BF)

            start_first(kind, 0)
            keep(kind).start()
        pass_on(DOWN, 0)

    def stage2():
        for kind in (GATE, UP):
            pass_on(kind, 0)
        rest(DOWN, 0)
        finish(DOWN, 0)
        keep(DOWN).wait()
        start_first(DOWN, 1)

    def stage3():
        for kind in (GATE, UP):
            rest(kind, 0)
            finish(kind, 0)
            keep(kind).wait()
            start_first(kind, 1)
            share(kind, 0).start()
        pass_on(DOWN, 1)

    def stage4():
        rest(DOWN, 1)
        finish(DOWN, 1)
        start_first(DOWN, 2)
        share(DOWN, 0).start()

    def stage5():
        for kind in (GATE, UP):
            pass_on(kind, 1)
        for kind in (GATE, UP):
            rest(kind, 1)
            share(kind, 1).start()
            share(kind, 2).start()

    def stage6():
        pass_on(DOWN, 2)
        rest(DOWN, 2)
        share(DOWN, 1).start()
        share(DOWN, 2).start()

    def stage7():
        for kind in (GATE, UP):
            finish(kind, 1)
            share(kind, 3).start()

    def stage8():
        finish(DOWN, 2)
        share(DOWN, 3).start()
        for kind in (GATE, UP, DOWN):
            for which in range(4):
                p = len(GATHER_ORDER[kind]) - 1
                ref = view(kind, p, SHARES[which], columns(SHARED, kind, 1 - core))
                arrived(ref, ds.at[kind, which], dr.at[kind, which])
        for kind in (GATE, UP):
            for by in (1, 3, 2):
                near(kind, by).wait_send()
        for kind in (GATE, UP, DOWN):
            for p in range(len(GATHER_ORDER[kind])):
                for n in range(2):
                    first(kind, p, n, 0).wait_send()
                    first(kind, p, n, 1).wait_send()
                    relay(kind, p, n).wait_send()
            for which in range(4):
                share(kind, which).wait_send()

    return [stage0, stage1, stage2, stage3, stage4, stage5, stage6, stage7, stage8]


def gather_scratch():
    dma = pltpu.SemaphoreType.DMA
    return [
        pltpu.VMEM((2, 3, D // 64, FF // 2), BF),
        pltpu.VMEM((2, D // 16, FF // 2), BF),
        dma((2, 3)),
        dma((2, 3)),
        dma((3, 3, 6)),
        dma((3, 3, 6)),
        dma((3, 4)),
        dma((3, 4)),
        dma((3,)),
    ]


VMEM, ANYWHERE = pl.BlockSpec(memory_space=pltpu.VMEM), pl.BlockSpec(memory_space=pl.ANY)


def gathered():
    wide = jax.ShapeDtypeStruct((4, 4, D // 16, FF), BF)
    return wide, wide, jax.ShapeDtypeStruct((4, 4, 4, FF // 64, D), BF)


def matrices(gate, up, down):
    return gate.reshape(D, FF), up.reshape(D, FF), down.reshape(FF, D)


SCATTER_ORDER = {GATE: (X, Y, Z), UP: (Y, X, Z), DOWN: (Z, X, Y)}
SPLIT = {GATE: 1280, UP: 1280, DOWN: 512}
COLS = {GATE: FF, UP: FF, DOWN: D}
BLOCKS = {
    GATE: ((4, 56), (1, 56), (1, 16)),
    UP: ((4, 56), (1, 56), (1, 16)),
    DOWN: ((16, 40), (4, 40), (1, 40)),
}
KINDS = (DOWN, GATE, UP)


def sums_of(phases):
    return (1,) if phases == (0,) else (1, 2)


def scatter_plan(phases, terms, outs, refs, carried=()):
    refs = list(refs)
    buf = {(k, p): [refs.pop(0) for _ in range(4)] for k in range(3) for p in phases}
    sums = sums_of(phases)
    wide = {(k, p): refs.pop(0) for k in range(3) for p in sums}
    stage = {(k, p): refs.pop(0) for k in range(3) for p in sums}
    own = {k: [refs.pop(0) for _ in range(3)] for k in range(3) if 0 in phases}
    ss, rs, ls, cs = refs
    core, at = place()

    def block(k, p, by):
        v = (at[SCATTER_ORDER[k][p]] + by) % 4
        if p:
            return stage[k, p].at[v]
        return terms[k].at[v] if k == GATE else terms[k].at[:, v]

    def part(k, n):
        return pl.ds(0, SPLIT[k]) if n == 0 else pl.ds(SPLIT[k], COLS[k] - SPLIT[k])

    def flow(k, p, n):
        from_left, from_right, left, right = buf[k, p]
        src, dst = {
            0: lambda: (block(k, p, 2).at[:, :, part(k, 0)], from_left),
            1: lambda: (block(k, p, 2).at[:, :, part(k, 1)], from_right),
            2: lambda: (block(k, p, 1).at[:, :, part(k, 1)], left.at[:, :, part(k, 1)]),
            3: lambda: (block(k, p, -1).at[:, :, part(k, 0)], right.at[:, :, part(k, 0)]),
            4: lambda: (from_left, left.at[:, :, part(k, 0)]),
            5: lambda: (from_right, right.at[:, :, part(k, 1)]),
        }[n]()
        to = moved(core, at, SCATTER_ORDER[k][p], (1, -1)[n % 2])
        sems = ss.at[k, p, n], rs.at[k, p, n]
        return pltpu.make_async_remote_copy(src, dst, *sems, device_id=to, device_id_type=MESH)

    def load(k, n):
        src = (lambda: block(k, 0, 1).at[:, :, part(k, 0)], lambda: block(k, 0, -1).at[:, :, part(k, 1)], lambda: block(k, 0, 0))[n]()
        return pltpu.make_async_copy(src, own[k][n], ls.at[k, n])

    def each(k, p, width, body):
        step = width if k == DOWN else 640
        count = width // step

        def one(i, carry):
            body(i // count, (i % count) * step, step)
            return carry

        lax.fori_loop(0, BLOCKS[k][p][0] * count, one, 0)

    def here(start, step):
        return pl.ds(pl.multiple_of(start, 128), step)

    def begin(k, p):
        for n in range(4):
            flow(k, p, n).start()
        if p == 0:
            for n in range(3):
                load(k, n).start()

    def middle(k, p):
        for n in range(2):
            flow(k, p, n).wait_recv()
            if p == 0:
                load(k, n).wait()
            come, before = buf[k, p][n], 0 if p == 0 or n == 0 else SPLIT[k]
            mine = own[k][n] if p == 0 else wide[k, p].at[(at[SCATTER_ORDER[k][p]] + (1, -1)[n]) % 4]

            def add(i, start, step, mine=mine, come=come, before=before):
                cols = here(start, step)
                come[i, :, cols] = (mine[i, :, here(start + before, step)].astype(F32) + come[i, :, cols].astype(F32)).astype(BF)

            each(k, p, SPLIT[k] if n == 0 else COLS[k] - SPLIT[k], add)
            flow(k, p, 4 + n).start()

    def end(k, p):
        left, right = buf[k, p][2:]
        for n in range(2, 6):
            flow(k, p, n).wait_recv()
        if p == 0:
            load(k, 2).wait()
        mine = own[k][2] if p == 0 else wide[k, p].at[at[SCATTER_ORDER[k][p]]]

        def add(i, start, step):
            cols = here(start, step)
            total = mine[i, :, cols].astype(F32) + left[i, :, cols].astype(F32) + right[i, :, cols].astype(F32)
            if p == 2:
                outs[k][:, cols] = total[: 40 if k == DOWN else 14].astype(BF)
            elif k != DOWN and p == 1:
                for z in range(4):
                    rows = jnp.concatenate([total[14 * z : 14 * z + 14], jnp.zeros((2, step), F32)], axis=0)
                    wide[k, 2][z, 0, :, cols] = rows
                    stage[k, 2][z, 0, :, cols] = rows.astype(BF)
            else:
                at_row = (i, 0) if k != DOWN or p == 1 else (i // 4, i % 4)
                wide[k, p + 1][(*at_row, slice(None), cols)] = total
                stage[k, p + 1][(*at_row, slice(None), cols)] = total.astype(BF)

        each(k, p, COLS[k], add)
        if p + 1 in phases:
            begin(k, p + 1)
        elif p == 0:
            for n in range(2):
                carry(k, n).start()

    def carry(k, n):
        here, there = (wide, stage)[n][k, 1], carried[3 * n + k]
        if 0 in phases:
            return pltpu.make_async_copy(here, there, cs.at[k, n])
        return pltpu.make_async_copy(there, here, cs.at[k, n])

    def enter():
        meet([moved(core, at, d, by) for d in (X, Y, Z) for by in (1, -1)])
        for k in KINDS:
            if 0 in phases:
                begin(k, 0)
            else:
                for n in range(2):
                    carry(k, 1 - n).start()

    def go_on():
        for k in KINDS:
            carry(k, 1).wait()
            begin(k, 1)
        for k in KINDS:
            carry(k, 0).wait()

    def leave():
        for k in KINDS:
            for p in phases:
                for n in range(6):
                    flow(k, p, n).wait_send()
            if phases == (0,):
                for n in range(2):
                    carry(k, n).wait()

    stages = [enter] if 0 in phases else [enter, go_on]
    for p in phases:
        stages += [functools.partial(middle, k, p) for k in KINDS]
        stages += [functools.partial(end, k, p) for k in KINDS]
    return [*stages, leave]


def scatter_scratch(phases):
    scratch = []
    for k in range(3):
        for p in phases:
            lead, rows = BLOCKS[k][p]
            for cols in (SPLIT[k], COLS[k] - SPLIT[k], COLS[k], COLS[k]):
                scratch.append(pltpu.VMEM((lead, rows, cols), BF))
    for kind in (F32, BF):
        for k in range(3):
            for p in sums_of(phases):
                lead, rows = BLOCKS[k][p]
                scratch.append(pltpu.VMEM((4, lead, rows, COLS[k]), kind))
    if 0 in phases:
        for k in range(3):
            lead, rows = BLOCKS[k][0]
            for cols in (SPLIT[k], COLS[k] - SPLIT[k], COLS[k]):
                scratch.append(pltpu.VMEM((lead, rows, cols), BF))
    dma = pltpu.SemaphoreType.DMA
    return [*scratch, dma((3, 3, 6)), dma((3, 3, 6)), dma((3, 3)), dma((3, 2))]


def carried_shapes():
    blocks = [(4, *BLOCKS[k][1], COLS[k]) for k in range(3)]
    return tuple(jax.ShapeDtypeStruct(shape, kind) for kind in (F32, BF) for shape in blocks)


def scattered():
    wide = jax.ShapeDtypeStruct((D // 64, FF), BF)
    return wide, wide, jax.ShapeDtypeStruct((FF // 64, D), BF)


def blocked(t_gate, t_up, t_down):
    return t_gate.reshape(4, 4, 56, FF), t_up.reshape(4, 4, 56, FF), t_down.reshape(16, 4, 40, D)


TOKENS, CHUNK = 2048, 512
GATHER_AT = ((2, 0), (3, 0), (5, 0), (7, 0))
FIRST_PHASE_AT = ((0, 0), *((2, 3), (3, 0), (3, 0)), *((7, 3), (7, 5), (7, 5)), (7, 5))
OTHER_PHASES_AT = ((0, 0), (0, 1), *[(1, 1)] * 3, *((2, 2), (3, 0), (3, 0)), *[(4, 0)] * 3, *[(4, 3)] * 3, (4, 3))
ALL_PHASES_AT = ((0, 0), *((3, 0), (3, 1), (4, 0)), *[(7, 2)] * 16)


def run(stages, places, number):
    for stage, (tile, chunk) in zip(stages, places, strict=True):
        if chunk == number:
            pl.when(pl.program_id(0) == tile)(stage)

ROWS = ((1,), (1,))
FIRST = ((0,), (0,))


def dot(a, b, over=((1,), (0,))):
    return lax.dot_general(a, b, (over, ((), ())), preferred_element_type=F32)


def norm(h):
    wide = h.astype(F32)
    scale = lax.rsqrt(jnp.mean(wide * wide, -1, keepdims=True) + 1e-6)
    return (wide * scale).astype(BF), scale


def chunks():
    return [slice(j, j + CHUNK) for j in range(0, FF, CHUNK)]


def forward_kernel(h_ref, *refs):
    given, refs = refs[:3], refs[3:]
    out_ref, first, second = refs[0], refs[1:4], refs[4:7]
    refs = refs[7:]
    count = len(gather_scratch())
    weights, sems = refs[2 * count : -1], refs[-1]
    now = gather_plan(0, given, first, refs[:count])
    later = gather_plan(1, given, second, refs[count : 2 * count], meeting=False)

    def bring(k, i):
        if k == DOWN:
            src, rows = first[k].at[i // 16, (i // 4) % 4, i % 4], FF // 64
        else:
            src, rows = first[k].at[i // 4, i % 4], D // 16
        return pltpu.make_async_copy(src, weights[k].at[pl.ds(pl.multiple_of(rows * i, 8), rows)], sems.at[k, i])

    def every(k, act):
        def one(i, carry):
            act(bring(k, i))
            return carry

        lax.fori_loop(0, 64 if k == DOWN else 16, one, 0)

    @pl.when(pl.program_id(0) == 0)
    def _():
        for stage in (*now[:2], later[0], now[2], later[1], now[3], later[2], *now[4:6], later[3], now[6], later[4], *now[7:]):
            stage()
        for k in range(3):
            every(k, lambda copy: copy.start())
        for k in range(3):
            every(k, lambda copy: copy.wait())

    gate_ref, up_ref, down_ref = weights
    h = h_ref[...]
    a, _ = norm(h)
    total = None
    for number, cols in enumerate(chunks()):
        run(later[5:], GATHER_AT, number)
        gate, up = dot(a, gate_ref[:, cols]), dot(a, up_ref[:, cols])
        act = (gate * jax.nn.sigmoid(gate) * up).astype(BF)
        more = dot(act, down_ref[cols, :])
        total = more if total is None else total + more
    out_ref[...] = h + total.astype(BF)


def hidden(a, by, cols, gate_ref, up_ref, down_ref, act_ref, by_gate_ref, by_up_ref):
    gate, up = dot(a, gate_ref[:, cols]), dot(a, up_ref[:, cols])
    by_act = dot(by, down_ref[cols, :], ROWS).astype(BF).astype(F32)
    sig = jax.nn.sigmoid(gate)
    silu = gate * sig
    act_ref[:, cols] = (silu * up).astype(BF)
    by_up = (by_act * silu).astype(BF)
    by_gate = (by_act * up * (sig + silu * (1 - sig))).astype(BF)
    by_up_ref[:, cols] = by_up
    by_gate_ref[:, cols] = by_gate


def norm_back(h, scale, by, by_a):
    by_a, wide = by_a.astype(BF).astype(F32), h.astype(F32)
    inner = jnp.mean(by_a * wide, -1, keepdims=True)
    return by + (by_a * scale - wide * (scale * scale * scale * inner)).astype(BF)


def backward_kernel(h_ref, by_ref, gate_ref, up_ref, down_ref, by_h_ref, a_ref, act_ref, by_gate_ref, by_up_ref):
    h, by = h_ref[...], by_ref[...]
    a, scale = norm(h)
    a_ref[...] = a
    for cols in chunks():
        hidden(a, by, cols, gate_ref, up_ref, down_ref, act_ref, by_gate_ref, by_up_ref)
    total = dot(by_gate_ref[...], gate_ref[...], ROWS) + dot(by_up_ref[...], up_ref[...], ROWS)
    by_h_ref[...] = norm_back(h, scale, by, total)


def inner_kernel(h_ref, by_ref, gate_ref, up_ref, down_ref, *refs):
    terms, (a_ref, act_ref, by_gate_ref, by_up_ref), carried = refs[:3], refs[3:7], refs[7:13]
    plan = scatter_plan((0,), terms, None, refs[13:], carried)
    a, _ = norm(h_ref[...])
    by = by_ref[...]
    a_ref[...] = a
    for number, cols in enumerate(chunks()):
        run(plan, FIRST_PHASE_AT, number)
        hidden(a, by, cols, gate_ref, up_ref, down_ref, act_ref, by_gate_ref, by_up_ref)
    run(plan, FIRST_PHASE_AT, len(chunks()))


def outer_kernel(h_ref, by_ref, by_gate_ref, by_up_ref, gate_ref, up_ref, *refs):
    terms, ready, out_ref, outs, refs = refs[:3], refs[3:6], refs[6], refs[7:10], refs[10:]
    plan = scatter_plan((0, 1, 2), terms, [out.at[0] for out in outs], refs)

    @pl.when(pl.program_id(0) == 0)
    def _():
        for k in range(3):
            outs[k][1] = ready[k][...]

    run(plan, ALL_PHASES_AT, 0)
    h = h_ref[...]
    _, scale = norm(h)
    total = dot(by_gate_ref[...], gate_ref[...], ROWS)
    run(plan, ALL_PHASES_AT, 1)
    total = total + dot(by_up_ref[...], up_ref[...], ROWS)
    out_ref[...] = norm_back(h, scale, by_ref[...], total)
    run(plan, ALL_PHASES_AT, 2)


def weights_kernel(hosts, a_ref, by_ref, act_ref, by_gate_ref, by_up_ref, *refs):
    plan, places = (), ()
    if hosts:
        plan, places = scatter_plan((1, 2), None, refs[9:12], refs[13:], refs[:6]), OTHER_PHASES_AT
        refs = refs[6:]
    t_gate_ref, t_up_ref, t_down_ref = refs[:3]
    turned = refs[6] if hosts else refs[3]

    @pl.when(pl.program_id(0) == 0)
    def _():
        turned[...] = a_ref[...].T

    run(plan, places, 0)
    t_down_ref[...] = dot(act_ref[...], by_ref[...], FIRST).astype(BF)
    run(plan, places, 1)
    t_gate_ref[...] = dot(turned[...], by_gate_ref[...]).astype(BF)
    run(plan, places, 2)
    t_up_ref[...] = dot(turned[...], by_up_ref[...]).astype(BF)
    run(plan, places, 3)


def whole(shape):
    return pl.BlockSpec(shape, lambda i: (0, 0), pipeline_mode=pl.Buffered(1))


def of_tokens(tile, cols):
    return pl.BlockSpec((tile, cols), lambda i: (i, 0))


def cost(matmuls):
    return pl.CostEstimate(flops=matmuls * 2 * TOKENS * D * FF, transcendentals=0, bytes_accessed=40_000_000)


def shaped(*shape):
    return jax.ShapeDtypeStruct(shape, BF)


def params(number=None):
    if number is None:
        return pltpu.CompilerParams(vmem_limit_bytes=BYTES)
    return pltpu.CompilerParams(collective_id=number, has_side_effects=True, vmem_limit_bytes=BYTES)


WEIGHTS = [whole((D, FF)), whole((D, FF)), whole((FF, D))]


def forward(h, shards):
    tile = TOKENS // 8
    h, *others = pl.pallas_call(
        forward_kernel,
        name="forward",
        grid=(TOKENS // tile,),
        out_shape=(shaped(TOKENS, D), *gathered(), *gathered()),
        in_specs=[of_tokens(tile, D), *[VMEM] * 3],
        out_specs=(of_tokens(tile, D), *[ANYWHERE] * 6),
        scratch_shapes=[
            *gather_scratch(),
            *gather_scratch(),
            pltpu.VMEM((D, FF), BF),
            pltpu.VMEM((D, FF), BF),
            pltpu.VMEM((FF, D), BF),
            pltpu.SemaphoreType.DMA((3, 64)),
        ],
        compiler_params=params(2),
        cost_estimate=cost(3),
    )(h, *shards)
    return h, matrices(*others[:3]), matrices(*others[3:])


def backward(h, by, weights):
    tile = TOKENS // 4
    return pl.pallas_call(
        backward_kernel,
        name="backward",
        grid=(TOKENS // tile,),
        out_shape=(shaped(TOKENS, D), shaped(TOKENS, D), *[shaped(TOKENS, FF)] * 3),
        in_specs=[of_tokens(tile, D), of_tokens(tile, D), *WEIGHTS],
        out_specs=(*[of_tokens(tile, D)] * 2, *[of_tokens(tile, FF)] * 3),
        compiler_params=params(),
        cost_estimate=cost(5),
    )(h, by, *weights)


def inner(h, by, weights, terms):
    tile = TOKENS // 8
    a, act, by_gate, by_up, *carried = pl.pallas_call(
        inner_kernel,
        name="inner",
        grid=(TOKENS // tile,),
        out_shape=(shaped(TOKENS, D), *[shaped(TOKENS, FF)] * 3, *carried_shapes()),
        in_specs=[of_tokens(tile, D), of_tokens(tile, D), *WEIGHTS, *[ANYWHERE] * 3],
        out_specs=(of_tokens(tile, D), *[of_tokens(tile, FF)] * 3, *[ANYWHERE] * 6),
        scratch_shapes=scatter_scratch((0,)),
        compiler_params=params(3),
        cost_estimate=cost(3),
    )(h, by, *weights, *blocked(*terms))
    return a, act, by_gate, by_up, carried


def outer(h, by, by_gate, by_up, weights, terms, ready):
    tile = TOKENS // 8
    by_h, *sums = pl.pallas_call(
        outer_kernel,
        name="outer",
        grid=(TOKENS // tile,),
        out_shape=(shaped(TOKENS, D), *(shaped(2, *like.shape) for like in scattered())),
        in_specs=[*[of_tokens(tile, D)] * 2, *[of_tokens(tile, FF)] * 2, *WEIGHTS[:2], *[ANYWHERE] * 3, *[VMEM] * 3],
        out_specs=(of_tokens(tile, D), *[VMEM] * 3),
        scratch_shapes=scatter_scratch((0, 1, 2)),
        compiler_params=params(4),
        cost_estimate=cost(2),
    )(h, by, by_gate, by_up, *weights[:2], *blocked(*terms), *ready)
    return by_h, sums


def weights_terms(a, by, act, by_gate, by_up, carried=()):
    side = pl.BlockSpec((TOKENS, CHUNK), lambda i: (0, i))
    hosts = bool(carried)
    t_gate, t_up, t_down, *sums = pl.pallas_call(
        functools.partial(weights_kernel, hosts),
        name="weights_sums" if hosts else "weights",
        grid=(FF // CHUNK,),
        out_shape=(shaped(D, FF), shaped(D, FF), shaped(FF, D), *(scattered() if hosts else ())),
        in_specs=[whole((TOKENS, D)), whole((TOKENS, D)), side, side, side, *[ANYWHERE] * len(carried)],
        out_specs=(
            pl.BlockSpec((D, CHUNK), lambda i: (0, i)),
            pl.BlockSpec((D, CHUNK), lambda i: (0, i)),
            pl.BlockSpec((CHUNK, D), lambda i: (i, 0)),
            *([VMEM] * 3 if hosts else ()),
        ),
        scratch_shapes=[pltpu.VMEM((D, TOKENS), BF), *(scatter_scratch((1, 2)) if hosts else ())],
        compiler_params=params(5 if hosts else None),
        cost_estimate=cost(3),
    )(a, by, act, by_gate, by_up, *carried)
    return (t_gate, t_up, t_down), sums


def local(x, dy, *shards):
    x, dy = x[0], dy[0]
    h, first, second = forward(x, shards)
    by_h, *saved = backward(h, dy, second)
    a, act, by_gate, by_up = saved
    terms, _ = weights_terms(a, dy, act, by_gate, by_up)
    a, act, by_gate, by_up, carried = inner(x, by_h, first, terms)
    terms, of_second = weights_terms(a, by_h, act, by_gate, by_up, carried)
    by_x, sums = outer(x, by_h, by_gate, by_up, first, terms, of_second)
    return (by_x[None], *sums)


def solution(mesh):
    tokens, rows = P(("rep", "dp")), P(None, "dp", None)
    return jax.shard_map(
        local,
        mesh=mesh,
        in_specs=(tokens, tokens, rows, rows, rows),
        out_specs=(tokens, *([P("rep", "dp", None)] * 3)),
        check_vma=False,
    )
```

```python
import functools

import jax
import jax.numpy as jnp
from jax import lax
from jax.experimental import pallas as pl
from jax.experimental.pallas import tpu as pltpu
from jax.sharding import PartitionSpec as P

MESH = pl.DeviceIdType.MESH
BF, F32 = jnp.bfloat16, jnp.float32
D, FF, LAYERS = 896, 2560, 2
X, Y, Z = 0, 1, 2
GATE, UP, DOWN = 0, 1, 2


def place():
    me = lax.axis_index("dp")
    return lax.axis_index("rep"), (me // 16, (me // 4) % 4, me % 4)


def moved(core, at, dim, by):
    to = [(v + by) % 4 if d == dim else v for d, v in enumerate(at)]
    return core, to[0] * 16 + to[1] * 4 + to[2]


def meet(devices):
    barrier = pltpu.get_barrier_semaphore()
    for device in devices:
        pl.semaphore_signal(barrier, inc=1, device_id=device, device_id_type=MESH)
    pl.semaphore_wait(barrier, len(devices))


BYTES = 63 * 1024 * 1024
GATHER_ORDER = {GATE: (Y, X), UP: (X, Y), DOWN: (X, Y, Z)}
WINDOW = {GATE: (1280, 1280), UP: (1280, 1280), DOWN: (384, 512)}
SHARED = {GATE: (1280, 1280), UP: (1280, 1280), DOWN: (512, 384)}


def gather_plan(l, given, outs, refs, meeting=True):
    zb, block, zs, zr, ms, mr, ds, dr, ls = refs
    core, at = place()
    partner = (1 - core, lax.axis_index("dp"))

    def columns(table, kind, of, part=None):
        step, width = table[kind]
        start = of * step
        if part is not None:
            width //= 2
            start = start + part * width
        return pl.ds(pl.multiple_of(start, 128), width)

    def view(kind, p, by, cols):
        order = GATHER_ORDER[kind]
        index = []
        for d in range(3 if kind == DOWN else 2):
            if d in order[:p]:
                index.append(slice(None))
            elif d == order[p]:
                index.append((at[d] + by) % 4)
            else:
                index.append(at[d])
        return outs[kind].at[(*index, slice(None), cols)]

    def mine(kind):
        cols = columns(WINDOW, kind, core)
        return given[kind].at[l, :, cols] if kind == DOWN else block.at[kind]

    def remote(src, dst, s, r, device):
        return pltpu.make_async_remote_copy(src, dst, s, r, device_id=device, device_id_type=MESH)

    def near(kind, by):
        src, sem = given[kind].at[l, :, columns(WINDOW, kind, core)], (kind, by - 1)
        return remote(src, zb.at[sem], zs.at[sem], zr.at[sem], moved(core, at, Z, by))

    def first(kind, p, n, part):
        dst = view(kind, p, 0, columns(WINDOW, kind, core, part))
        width = WINDOW[kind][1] // 2
        src = dst
        if p == 0 and kind == DOWN:
            src = given[kind].at[l, :, columns(WINDOW, kind, core, part)]
        elif p == 0:
            src = block.at[kind, :, pl.ds(part * width, width)]
        to = moved(core, at, GATHER_ORDER[kind][p], (1, -1)[n])
        which = n if part == n else 4 + n
        return remote(src, dst, ms.at[kind, p, which], mr.at[kind, p, which], to)

    def relay(kind, p, n):
        by = (1, -1)[n]
        half = view(kind, p, -by, columns(WINDOW, kind, core, n))
        to = moved(core, at, GATHER_ORDER[kind][p], by)
        return remote(half, half, ms.at[kind, p, 2 + n], mr.at[kind, p, 2 + n], to)

    SHARES = (0, 1, 3, 2)

    def share(kind, which):
        ref = view(kind, len(GATHER_ORDER[kind]) - 1, SHARES[which], columns(SHARED, kind, core))
        return remote(ref, ref, ds.at[kind, which], dr.at[kind, which], partner)

    def keep(kind):
        return pltpu.make_async_copy(mine(kind), view(kind, 0, 0, columns(WINDOW, kind, core)), ls.at[kind])

    def arrived(ref, s, r):
        remote(ref, ref, s, r, partner).wait_recv()

    def start_first(kind, p):
        for part in (0, 1):
            for n in range(2):
                first(kind, p, n, n if part == 0 else 1 - n).start()

    def pass_on(kind, p):
        for n in range(2):
            ref = view(kind, p, -(1, -1)[n], columns(WINDOW, kind, core, n))
            arrived(ref, ms.at[kind, p, n], mr.at[kind, p, n])
            relay(kind, p, n).start()

    def rest(kind, p):
        for n in range(2):
            ref = view(kind, p, -(1, -1)[n], columns(WINDOW, kind, core, 1 - n))
            arrived(ref, ms.at[kind, p, 4 + n], mr.at[kind, p, 4 + n])

    def finish(kind, p):
        for n in range(2):
            arrived(view(kind, p, 2, columns(WINDOW, kind, core, n)), ms.at[kind, p, 2 + n], mr.at[kind, p, 2 + n])

    def stage0():
        if meeting:
            meet([moved(core, at, d, by) for d in (X, Y, Z) for by in (1, 2, -1) if by != 2 or d == Z] + [partner])
        for kind in (GATE, UP):
            for by in (1, 3, 2):
                near(kind, by).start()
        start_first(DOWN, 0)
        keep(DOWN).start()

    def stage1():
        for kind in (GATE, UP):
            for n in range(3):
                arrived(zb.at[kind, n], zs.at[kind, n], zr.at[kind, n])
            come = [given[kind][l, :, columns(WINDOW, kind, core)].astype(F32)]
            come += [zb[kind, n].astype(F32) for n in range(3)]
            for z in range(4):

                @pl.when(at[Z] == z)
                def _(z=z, come=come, kind=kind):
                    block[kind] = jnp.concatenate([come[(z - row) % 4] for row in range(4)], axis=0).astype(BF)

            start_first(kind, 0)
            keep(kind).start()
        pass_on(DOWN, 0)

    def stage2():
        for kind in (GATE, UP):
            pass_on(kind, 0)
        rest(DOWN, 0)
        finish(DOWN, 0)
        keep(DOWN).wait()
        start_first(DOWN, 1)

    def stage3():
        for kind in (GATE, UP):
            rest(kind, 0)
            finish(kind, 0)
            keep(kind).wait()
            start_first(kind, 1)
            share(kind, 0).start()
        pass_on(DOWN, 1)

    def stage4():
        rest(DOWN, 1)
        finish(DOWN, 1)
        start_first(DOWN, 2)
        share(DOWN, 0).start()

    def stage5():
        for kind in (GATE, UP):
            pass_on(kind, 1)
        for kind in (GATE, UP):
            rest(kind, 1)
            share(kind, 1).start()
            share(kind, 2).start()

    def stage6():
        pass_on(DOWN, 2)
        rest(DOWN, 2)
        share(DOWN, 1).start()
        share(DOWN, 2).start()

    def stage7():
        for kind in (GATE, UP):
            finish(kind, 1)
            share(kind, 3).start()

    def stage8():
        finish(DOWN, 2)
        share(DOWN, 3).start()
        for kind in (GATE, UP, DOWN):
            for which in range(4):
                p = len(GATHER_ORDER[kind]) - 1
                ref = view(kind, p, SHARES[which], columns(SHARED, kind, 1 - core))
                arrived(ref, ds.at[kind, which], dr.at[kind, which])
        for kind in (GATE, UP):
            for by in (1, 3, 2):
                near(kind, by).wait_send()
        for kind in (GATE, UP, DOWN):
            for p in range(len(GATHER_ORDER[kind])):
                for n in range(2):
                    first(kind, p, n, 0).wait_send()
                    first(kind, p, n, 1).wait_send()
                    relay(kind, p, n).wait_send()
            for which in range(4):
                share(kind, which).wait_send()

    return [stage0, stage1, stage2, stage3, stage4, stage5, stage6, stage7, stage8]


def gather_scratch():
    dma = pltpu.SemaphoreType.DMA
    return [
        pltpu.VMEM((2, 3, D // 64, FF // 2), BF),
        pltpu.VMEM((2, D // 16, FF // 2), BF),
        dma((2, 3)),
        dma((2, 3)),
        dma((3, 3, 6)),
        dma((3, 3, 6)),
        dma((3, 4)),
        dma((3, 4)),
        dma((3,)),
    ]


VMEM, ANYWHERE = pl.BlockSpec(memory_space=pltpu.VMEM), pl.BlockSpec(memory_space=pl.ANY)


def gathered():
    wide = jax.ShapeDtypeStruct((4, 4, D // 16, FF), BF)
    return wide, wide, jax.ShapeDtypeStruct((4, 4, 4, FF // 64, D), BF)


def matrices(gate, up, down):
    return gate.reshape(D, FF), up.reshape(D, FF), down.reshape(FF, D)


SCATTER_ORDER = {GATE: (X, Y, Z), UP: (Y, X, Z), DOWN: (Z, X, Y)}
SPLIT = {GATE: 1280, UP: 1280, DOWN: 512}
COLS = {GATE: FF, UP: FF, DOWN: D}
BLOCKS = {
    GATE: ((4, 56), (1, 56), (1, 16)),
    UP: ((4, 56), (1, 56), (1, 16)),
    DOWN: ((16, 40), (4, 40), (1, 40)),
}
KINDS = (DOWN, GATE, UP)


def sums_of(phases):
    return (1,) if phases == (0,) else (1, 2)


def scatter_plan(phases, terms, outs, refs, carried=()):
    refs = list(refs)
    buf = {(k, p): [refs.pop(0) for _ in range(4)] for k in range(3) for p in phases}
    sums = sums_of(phases)
    wide = {(k, p): refs.pop(0) for k in range(3) for p in sums}
    stage = {(k, p): refs.pop(0) for k in range(3) for p in sums}
    own = {k: [refs.pop(0) for _ in range(3)] for k in range(3) if 0 in phases}
    ss, rs, ls, cs = refs
    core, at = place()

    def block(k, p, by):
        v = (at[SCATTER_ORDER[k][p]] + by) % 4
        if p:
            return stage[k, p].at[v]
        return terms[k].at[v] if k == GATE else terms[k].at[:, v]

    def part(k, n):
        return pl.ds(0, SPLIT[k]) if n == 0 else pl.ds(SPLIT[k], COLS[k] - SPLIT[k])

    def flow(k, p, n):
        from_left, from_right, left, right = buf[k, p]
        src, dst = {
            0: lambda: (block(k, p, 2).at[:, :, part(k, 0)], from_left),
            1: lambda: (block(k, p, 2).at[:, :, part(k, 1)], from_right),
            2: lambda: (block(k, p, 1).at[:, :, part(k, 1)], left.at[:, :, part(k, 1)]),
            3: lambda: (block(k, p, -1).at[:, :, part(k, 0)], right.at[:, :, part(k, 0)]),
            4: lambda: (from_left, left.at[:, :, part(k, 0)]),
            5: lambda: (from_right, right.at[:, :, part(k, 1)]),
        }[n]()
        to = moved(core, at, SCATTER_ORDER[k][p], (1, -1)[n % 2])
        sems = ss.at[k, p, n], rs.at[k, p, n]
        return pltpu.make_async_remote_copy(src, dst, *sems, device_id=to, device_id_type=MESH)

    def load(k, n):
        src = (lambda: block(k, 0, 1).at[:, :, part(k, 0)], lambda: block(k, 0, -1).at[:, :, part(k, 1)], lambda: block(k, 0, 0))[n]()
        return pltpu.make_async_copy(src, own[k][n], ls.at[k, n])

    def each(k, p, width, body):
        step = width if k == DOWN else 640
        count = width // step

        def one(i, carry):
            body(i // count, (i % count) * step, step)
            return carry

        lax.fori_loop(0, BLOCKS[k][p][0] * count, one, 0)

    def here(start, step):
        return pl.ds(pl.multiple_of(start, 128), step)

    def begin(k, p):
        for n in range(4):
            flow(k, p, n).start()
        if p == 0:
            for n in range(3):
                load(k, n).start()

    def middle(k, p):
        for n in range(2):
            flow(k, p, n).wait_recv()
            if p == 0:
                load(k, n).wait()
            come, before = buf[k, p][n], 0 if p == 0 or n == 0 else SPLIT[k]
            mine = own[k][n] if p == 0 else wide[k, p].at[(at[SCATTER_ORDER[k][p]] + (1, -1)[n]) % 4]

            def add(i, start, step, mine=mine, come=come, before=before):
                cols = here(start, step)
                come[i, :, cols] = (mine[i, :, here(start + before, step)].astype(F32) + come[i, :, cols].astype(F32)).astype(BF)

            each(k, p, SPLIT[k] if n == 0 else COLS[k] - SPLIT[k], add)
            flow(k, p, 4 + n).start()

    def end(k, p):
        left, right = buf[k, p][2:]
        for n in range(2, 6):
            flow(k, p, n).wait_recv()
        if p == 0:
            load(k, 2).wait()
        mine = own[k][2] if p == 0 else wide[k, p].at[at[SCATTER_ORDER[k][p]]]

        def add(i, start, step):
            cols = here(start, step)
            total = mine[i, :, cols].astype(F32) + left[i, :, cols].astype(F32) + right[i, :, cols].astype(F32)
            if p == 2:
                outs[k][:, cols] = total[: 40 if k == DOWN else 14].astype(BF)
            elif k != DOWN and p == 1:
                for z in range(4):
                    rows = jnp.concatenate([total[14 * z : 14 * z + 14], jnp.zeros((2, step), F32)], axis=0)
                    wide[k, 2][z, 0, :, cols] = rows
                    stage[k, 2][z, 0, :, cols] = rows.astype(BF)
            else:
                at_row = (i, 0) if k != DOWN or p == 1 else (i // 4, i % 4)
                wide[k, p + 1][(*at_row, slice(None), cols)] = total
                stage[k, p + 1][(*at_row, slice(None), cols)] = total.astype(BF)

        each(k, p, COLS[k], add)
        if p + 1 in phases:
            begin(k, p + 1)
        elif p == 0:
            for n in range(2):
                carry(k, n).start()

    def carry(k, n):
        here, there = (wide, stage)[n][k, 1], carried[3 * n + k]
        if 0 in phases:
            return pltpu.make_async_copy(here, there, cs.at[k, n])
        return pltpu.make_async_copy(there, here, cs.at[k, n])

    def enter():
        meet([moved(core, at, d, by) for d in (X, Y, Z) for by in (1, -1)])
        for k in KINDS:
            if 0 in phases:
                begin(k, 0)
            else:
                for n in range(2):
                    carry(k, 1 - n).start()

    def go_on():
        for k in KINDS:
            carry(k, 1).wait()
            begin(k, 1)
        for k in KINDS:
            carry(k, 0).wait()

    def leave():
        for k in KINDS:
            for p in phases:
                for n in range(6):
                    flow(k, p, n).wait_send()
            if phases == (0,):
                for n in range(2):
                    carry(k, n).wait()

    stages = [enter] if 0 in phases else [enter, go_on]
    for p in phases:
        stages += [functools.partial(middle, k, p) for k in KINDS]
        stages += [functools.partial(end, k, p) for k in KINDS]
    return [*stages, leave]


def scatter_scratch(phases):
    scratch = []
    for k in range(3):
        for p in phases:
            lead, rows = BLOCKS[k][p]
            for cols in (SPLIT[k], COLS[k] - SPLIT[k], COLS[k], COLS[k]):
                scratch.append(pltpu.VMEM((lead, rows, cols), BF))
    for kind in (F32, BF):
        for k in range(3):
            for p in sums_of(phases):
                lead, rows = BLOCKS[k][p]
                scratch.append(pltpu.VMEM((4, lead, rows, COLS[k]), kind))
    if 0 in phases:
        for k in range(3):
            lead, rows = BLOCKS[k][0]
            for cols in (SPLIT[k], COLS[k] - SPLIT[k], COLS[k]):
                scratch.append(pltpu.VMEM((lead, rows, cols), BF))
    dma = pltpu.SemaphoreType.DMA
    return [*scratch, dma((3, 3, 6)), dma((3, 3, 6)), dma((3, 3)), dma((3, 2))]


def carried_shapes():
    blocks = [(4, *BLOCKS[k][1], COLS[k]) for k in range(3)]
    return tuple(jax.ShapeDtypeStruct(shape, kind) for kind in (F32, BF) for shape in blocks)


def scattered():
    wide = jax.ShapeDtypeStruct((D // 64, FF), BF)
    return wide, wide, jax.ShapeDtypeStruct((FF // 64, D), BF)


def blocked(t_gate, t_up, t_down):
    return t_gate.reshape(4, 4, 56, FF), t_up.reshape(4, 4, 56, FF), t_down.reshape(16, 4, 40, D)


TOKENS, CHUNK = 2048, 512
GATHER_AT = ((2, 0), (3, 0), (5, 0), (7, 0))
FIRST_PHASE_AT = ((0, 0), *((4, 0), (4, 3), (4, 3)), *((7, 5), (7, 5), (7, 5)), (7, 5))
OTHER_PHASES_AT = ((0, 0), (0, 1), *[(1, 1)] * 3, *((2, 2), (3, 0), (3, 0)), *[(4, 0)] * 3, *[(4, 3)] * 3, (4, 3))
ALL_PHASES_AT = ((0, 0), *((3, 0), (3, 1), (4, 0)), *[(7, 2)] * 16)


def run(stages, places, number):
    for stage, (tile, chunk) in zip(stages, places, strict=True):
        if chunk == number:
            pl.when(pl.program_id(0) == tile)(stage)

ROWS = ((1,), (1,))
FIRST = ((0,), (0,))


def dot(a, b, over=((1,), (0,))):
    return lax.dot_general(a, b, (over, ((), ())), preferred_element_type=F32)


def norm(h):
    wide = h.astype(F32)
    scale = lax.rsqrt(jnp.mean(wide * wide, -1, keepdims=True) + 1e-6)
    return (wide * scale).astype(BF), scale


def chunks():
    return [slice(j, j + CHUNK) for j in range(0, FF, CHUNK)]


def forward_kernel(h_ref, *refs):
    given, refs = refs[:3], refs[3:]
    out_ref, a_ref, keep_gate_ref, keep_up_ref, first, second = *refs[:4], refs[4:7], refs[7:10]
    refs = refs[10:]
    count = len(gather_scratch())
    weights, sems = refs[2 * count : -1], refs[-1]
    now = gather_plan(0, given, first, refs[:count])
    later = gather_plan(1, given, second, refs[count : 2 * count], meeting=False)

    def bring(k, i):
        if k == DOWN:
            src, rows = first[k].at[i // 16, (i // 4) % 4, i % 4], FF // 64
        else:
            src, rows = first[k].at[i // 4, i % 4], D // 16
        return pltpu.make_async_copy(src, weights[k].at[pl.ds(pl.multiple_of(rows * i, 8), rows)], sems.at[k, i])

    def every(k, act):
        def one(i, carry):
            act(bring(k, i))
            return carry

        lax.fori_loop(0, 64 if k == DOWN else 16, one, 0)

    @pl.when(pl.program_id(0) == 0)
    def _():
        for stage in (*now[:2], later[0], now[2], later[1], now[3], later[2], *now[4:6], later[3], now[6], later[4], *now[7:]):
            stage()
        for k in range(3):
            every(k, lambda copy: copy.start())
        for k in range(3):
            every(k, lambda copy: copy.wait())

    gate_ref, up_ref, down_ref = weights
    h = h_ref[...]
    a, _ = norm(h)
    a_ref[...] = a
    total = None
    for number, cols in enumerate(chunks()):
        run(later[5:], GATHER_AT, number)
        gate, up = dot(a, gate_ref[:, cols]), dot(a, up_ref[:, cols])
        keep_gate_ref[:, cols] = gate
        keep_up_ref[:, cols] = up
        act = (gate * jax.nn.sigmoid(gate) * up).astype(BF)
        more = dot(act, down_ref[cols, :])
        total = more if total is None else total + more
    out_ref[...] = h + total.astype(BF)


def hidden(gate, up, by, cols, down_ref, act_ref, by_gate_ref, by_up_ref):
    by_act = dot(by, down_ref[cols, :], ROWS).astype(BF).astype(F32)
    sig = jax.nn.sigmoid(gate)
    silu = gate * sig
    act_ref[:, cols] = (silu * up).astype(BF)
    by_up = (by_act * silu).astype(BF)
    by_gate = (by_act * up * (sig + silu * (1 - sig))).astype(BF)
    by_up_ref[:, cols] = by_up
    by_gate_ref[:, cols] = by_gate


def norm_back(h, scale, by, by_a):
    by_a, wide = by_a.astype(BF).astype(F32), h.astype(F32)
    inner = jnp.mean(by_a * wide, -1, keepdims=True)
    return by + (by_a * scale - wide * (scale * scale * scale * inner)).astype(BF)


def backward_kernel(h_ref, by_ref, gate_ref, up_ref, down_ref, by_h_ref, a_ref, act_ref, by_gate_ref, by_up_ref):
    h, by = h_ref[...], by_ref[...]
    a, scale = norm(h)
    a_ref[...] = a
    for cols in chunks():
        gate, up = dot(a, gate_ref[:, cols]), dot(a, up_ref[:, cols])
        hidden(gate, up, by, cols, down_ref, act_ref, by_gate_ref, by_up_ref)
    total = dot(by_gate_ref[...], gate_ref[...], ROWS) + dot(by_up_ref[...], up_ref[...], ROWS)
    by_h_ref[...] = norm_back(h, scale, by, total)


def inner_kernel(by_ref, gate_ref, up_ref, down_ref, *refs):
    terms, results, carried = refs[:3], refs[3:6], refs[6:12]
    plan = scatter_plan((0,), terms, None, refs[12:], carried)
    by = by_ref[...]
    for number, cols in enumerate(chunks()):
        run(plan, FIRST_PHASE_AT, number)
        hidden(gate_ref[:, cols], up_ref[:, cols], by, cols, down_ref, *results)
    run(plan, FIRST_PHASE_AT, len(chunks()))


def outer_kernel(h_ref, by_ref, by_gate_ref, by_up_ref, gate_ref, up_ref, *refs):
    terms, ready, out_ref, outs, refs = refs[:3], refs[3:6], refs[6], refs[7:10], refs[10:]
    plan = scatter_plan((0, 1, 2), terms, [out.at[0] for out in outs], refs)

    @pl.when(pl.program_id(0) == 0)
    def _():
        for k in range(3):
            outs[k][1] = ready[k][...]

    run(plan, ALL_PHASES_AT, 0)
    h = h_ref[...]
    _, scale = norm(h)
    total = dot(by_gate_ref[...], gate_ref[...], ROWS)
    run(plan, ALL_PHASES_AT, 1)
    total = total + dot(by_up_ref[...], up_ref[...], ROWS)
    out_ref[...] = norm_back(h, scale, by_ref[...], total)
    run(plan, ALL_PHASES_AT, 2)


def weights_kernel(hosts, a_ref, by_ref, act_ref, by_gate_ref, by_up_ref, *refs):
    plan, places = (), ()
    if hosts:
        plan, places = scatter_plan((1, 2), None, refs[9:12], refs[13:], refs[:6]), OTHER_PHASES_AT
        refs = refs[6:]
    t_gate_ref, t_up_ref, t_down_ref = refs[:3]
    turned = refs[6] if hosts else refs[3]

    @pl.when(pl.program_id(0) == 0)
    def _():
        turned[...] = a_ref[...].T

    run(plan, places, 0)
    t_down_ref[...] = dot(act_ref[...], by_ref[...], FIRST).astype(BF)
    run(plan, places, 1)
    t_gate_ref[...] = dot(turned[...], by_gate_ref[...]).astype(BF)
    run(plan, places, 2)
    t_up_ref[...] = dot(turned[...], by_up_ref[...]).astype(BF)
    run(plan, places, 3)


def whole(shape):
    return pl.BlockSpec(shape, lambda i: (0, 0), pipeline_mode=pl.Buffered(1))


def of_tokens(tile, cols):
    return pl.BlockSpec((tile, cols), lambda i: (i, 0))


def cost(matmuls):
    return pl.CostEstimate(flops=matmuls * 2 * TOKENS * D * FF, transcendentals=0, bytes_accessed=40_000_000)


def shaped(*shape):
    return jax.ShapeDtypeStruct(shape, BF)


def params(number=None):
    if number is None:
        return pltpu.CompilerParams(vmem_limit_bytes=BYTES)
    return pltpu.CompilerParams(collective_id=number, has_side_effects=True, vmem_limit_bytes=BYTES)


WEIGHTS = [whole((D, FF)), whole((D, FF)), whole((FF, D))]


def forward(h, shards):
    tile = TOKENS // 8
    h, a, gate, up, *others = pl.pallas_call(
        forward_kernel,
        name="forward",
        grid=(TOKENS // tile,),
        out_shape=(*[shaped(TOKENS, D)] * 2, *[jax.ShapeDtypeStruct((TOKENS, FF), F32)] * 2, *gathered(), *gathered()),
        in_specs=[of_tokens(tile, D), *[VMEM] * 3],
        out_specs=(*[of_tokens(tile, D)] * 2, *[of_tokens(tile, FF)] * 2, *[ANYWHERE] * 6),
        scratch_shapes=[
            *gather_scratch(),
            *gather_scratch(),
            pltpu.VMEM((D, FF), BF),
            pltpu.VMEM((D, FF), BF),
            pltpu.VMEM((FF, D), BF),
            pltpu.SemaphoreType.DMA((3, 64)),
        ],
        compiler_params=params(2),
        cost_estimate=cost(3),
    )(h, *shards)
    return h, (a, gate, up), matrices(*others[:3]), matrices(*others[3:])


def backward(h, by, weights):
    tile = TOKENS // 4
    return pl.pallas_call(
        backward_kernel,
        name="backward",
        grid=(TOKENS // tile,),
        out_shape=(shaped(TOKENS, D), shaped(TOKENS, D), *[shaped(TOKENS, FF)] * 3),
        in_specs=[of_tokens(tile, D), of_tokens(tile, D), *WEIGHTS],
        out_specs=(*[of_tokens(tile, D)] * 2, *[of_tokens(tile, FF)] * 3),
        compiler_params=params(),
        cost_estimate=cost(5),
    )(h, by, *weights)


def inner(by, gate, up, w_down, terms):
    tile = TOKENS // 8
    act, by_gate, by_up, *carried = pl.pallas_call(
        inner_kernel,
        name="inner",
        grid=(TOKENS // tile,),
        out_shape=(*[shaped(TOKENS, FF)] * 3, *carried_shapes()),
        in_specs=[of_tokens(tile, D), *[of_tokens(tile, FF)] * 2, WEIGHTS[2], *[ANYWHERE] * 3],
        out_specs=(*[of_tokens(tile, FF)] * 3, *[ANYWHERE] * 6),
        scratch_shapes=scatter_scratch((0,)),
        compiler_params=params(3),
        cost_estimate=cost(1),
    )(by, gate, up, w_down, *blocked(*terms))
    return act, by_gate, by_up, carried


def outer(h, by, by_gate, by_up, weights, terms, ready):
    tile = TOKENS // 8
    by_h, *sums = pl.pallas_call(
        outer_kernel,
        name="outer",
        grid=(TOKENS // tile,),
        out_shape=(shaped(TOKENS, D), *(shaped(2, *like.shape) for like in scattered())),
        in_specs=[*[of_tokens(tile, D)] * 2, *[of_tokens(tile, FF)] * 2, *WEIGHTS[:2], *[ANYWHERE] * 3, *[VMEM] * 3],
        out_specs=(of_tokens(tile, D), *[VMEM] * 3),
        scratch_shapes=scatter_scratch((0, 1, 2)),
        compiler_params=params(4),
        cost_estimate=cost(2),
    )(h, by, by_gate, by_up, *weights[:2], *blocked(*terms), *ready)
    return by_h, sums


def weights_terms(a, by, act, by_gate, by_up, carried=()):
    side = pl.BlockSpec((TOKENS, CHUNK), lambda i: (0, i))
    hosts = bool(carried)
    t_gate, t_up, t_down, *sums = pl.pallas_call(
        functools.partial(weights_kernel, hosts),
        name="weights_sums" if hosts else "weights",
        grid=(FF // CHUNK,),
        out_shape=(shaped(D, FF), shaped(D, FF), shaped(FF, D), *(scattered() if hosts else ())),
        in_specs=[whole((TOKENS, D)), whole((TOKENS, D)), side, side, side, *[ANYWHERE] * len(carried)],
        out_specs=(
            pl.BlockSpec((D, CHUNK), lambda i: (0, i)),
            pl.BlockSpec((D, CHUNK), lambda i: (0, i)),
            pl.BlockSpec((CHUNK, D), lambda i: (i, 0)),
            *([VMEM] * 3 if hosts else ()),
        ),
        scratch_shapes=[pltpu.VMEM((D, TOKENS), BF), *(scatter_scratch((1, 2)) if hosts else ())],
        compiler_params=params(5 if hosts else None),
        cost_estimate=cost(3),
    )(a, by, act, by_gate, by_up, *carried)
    return (t_gate, t_up, t_down), sums


def local(x, dy, *shards):
    x, dy = x[0], dy[0]
    h, (a0, gate, up), first, second = forward(x, shards)
    by_h, *saved = backward(h, dy, second)
    a, act, by_gate, by_up = saved
    terms, _ = weights_terms(a, dy, act, by_gate, by_up)
    act, by_gate, by_up, carried = inner(by_h, gate, up, first[2], terms)
    terms, of_second = weights_terms(a0, by_h, act, by_gate, by_up, carried)
    by_x, sums = outer(x, by_h, by_gate, by_up, first, terms, of_second)
    return (by_x[None], *sums)


def solution(mesh):
    tokens, rows = P(("rep", "dp")), P(None, "dp", None)
    return jax.shard_map(
        local,
        mesh=mesh,
        in_specs=(tokens, tokens, rows, rows, rows),
        out_specs=(tokens, *([P("rep", "dp", None)] * 3)),
        check_vma=False,
    )
```
